128 devices in a mesh: leaf: 32 (over x, y, core), nbr: 4 (over z).
Axes of the slice: x: 4, y: 4, z: 4, core: 2. Of those that a mesh axis runs over, the one named last changes fastest.
Arguments:
- points: bfloat16 [1024, 32, 512], P('leaf'), may hold values from -1.1953125 to 1.1953125
- charges: bfloat16 [1024, 64, 512], P('leaf'), may hold values from -1.5 to 1.5
- projection: bfloat16 [1024, 256, 512], P('leaf', 'nbr'), may hold values from -0.25 to 0.25
- skeleton_index: int32 [1024, 256], P('leaf'), may hold values from 0 to 511, as said below
- near_ids: int32 [1024, 8], P('leaf', 'nbr'), may hold values from 0 to 1023, as said below
- far_ids: int32 [1024, 16], P('leaf', 'nbr'), may hold values from 0 to 1023, as said below
Outputs:
- potentials: float32 [1024, 64, 512], P('leaf', None, 'nbr')
The draws below stay inside these ranges and needn't reach their ends.
Inputs may be any that keep to these rules, and one draw needn't show every extreme that they name: `skeleton_index`: each row holds 256 different point numbers of its leaf. `near_ids`: take the rows of one block of 32 leaves (leaf numbers k * 32 to k * 32 + 31) and one of the 4 equal groups of columns: at most 3 of its entries name leaves of any one such block, and some block is named exactly 3 times. `far_ids`: take the rows of one block of 32 leaves and one of the 4 equal groups of columns: at most 5 of its entries name leaves of any one such block, and some block is named exactly 5 times.
All inputs are finite; a program needn't handle non-finite values.
Results may differ from the reference program's by a relative error of at most 0.002.
Values may be sent and summed in bfloat16 or wider, within the bound.
A program may use at most 128 MiB of HBM per device.

```python
import jax
import jax.numpy as jnp
from jax import lax

DIM = 32
RHS = 64
LEAF = 512
SKEL = 256
NEAR = 8
FAR = 16
LEAF_DEV = 32
NLEAF = 1024
CAP_NEAR = 3
CAP_FAR = 5
N_LEAF = 32
N_NBR = 4


def spread_lists(base_key, per_device, capacity, far_side):
    entry_count = LEAF_DEV * per_device
    slot_count = N_LEAF * capacity
    owner_slot = jnp.arange(slot_count, dtype=jnp.int32) // capacity

    def list_block(flat_index):
        home_leaf = flat_index // N_NBR
        block_key = jax.random.fold_in(base_key, flat_index)
        key_jitter, key_order, key_local = jax.random.split(block_key, 3)
        circle_gap = (owner_slot - home_leaf) % N_LEAF
        distance = jnp.minimum(circle_gap, N_LEAF - circle_gap)
        jitter = jax.random.randint(key_jitter, (slot_count,), 0, 1024)
        if far_side:
            lift_score = 2048 * jnp.minimum(distance, 3)
            forced_owner = (home_leaf + N_LEAF // 2) % N_LEAF
        else:
            lift_score = 2048 * jnp.maximum(0, 3 - distance)
            forced_owner = (home_leaf + 1) % N_LEAF
        scores = jnp.where(owner_slot == forced_owner, 8192, jitter + lift_score)
        scores = scores * slot_count + jnp.arange(slot_count, dtype=jnp.int32)
        _, chosen = lax.top_k(scores, entry_count)
        chosen = jax.random.permutation(key_order, chosen)
        local_leaf = jax.random.randint(key_local, (entry_count,), 0, LEAF_DEV)
        return (chosen // capacity * LEAF_DEV + local_leaf).astype(jnp.int32).reshape(LEAF_DEV, per_device)
    blocks = jax.vmap(list_block)(jnp.arange(N_LEAF * N_NBR, dtype=jnp.int32))
    blocks = blocks.reshape(N_LEAF, N_NBR, LEAF_DEV, per_device).transpose(0, 2, 1, 3)
    return blocks.reshape(NLEAF, N_NBR * per_device)


def draw_near_ids(key, part):
    return spread_lists(jax.random.fold_in(key, 11), NEAR // N_NBR, CAP_NEAR, False)


def draw_far_ids(key, part):
    return spread_lists(jax.random.fold_in(key, 17), FAR // N_NBR, CAP_FAR, True)


def draw_skeleton_index(key, part):
    scores = jax.random.randint(jax.random.fold_in(key, 13), (NLEAF, LEAF), 0, 65536)
    scores = scores * LEAF + jnp.arange(LEAF, dtype=jnp.int32)[None, :]
    _, chosen = lax.top_k(scores, SKEL)
    return chosen.astype(jnp.int32)


def levels(own_key, dims, shards, low, largest):
    level, own = 1.0, jax.random.fold_in(own_key, 6)
    for axis_at, parts in shards:
        steps = jnp.exp(jax.random.uniform(jax.random.fold_in(own, axis_at), (parts,), jnp.float32, low / len(shards), largest / len(shards)))
        level = level * jnp.repeat(steps, dims[axis_at] // parts).reshape([-1 if axis == axis_at else 1 for axis in range(len(dims))])
    return level


def noise(key, shape, scale, reach, cuts=(), held_as=jnp.bfloat16):
    values = jax.random.normal(key, shape, jnp.float32) * scale
    if len(cuts) > 0:
        values = levels(key, shape, cuts, -0.22, 0.18) * values
    return jnp.clip(values, min=-reach, max=reach).astype(held_as)


def setup_inputs(seed: int = 0) -> dict:
    seeds = jax.random.split(jax.random.key(seed), 7)
    points = noise(seeds[0], (NLEAF, DIM, LEAF), 0.2, 1.1953125, ((0, 32),))
    charges = noise(seeds[1], (NLEAF, RHS, LEAF), 0.25, 1.5, ((0, 32),))
    projection = noise(seeds[2], (NLEAF, SKEL, LEAF), LEAF ** -0.5, 0.25, ((0, 32), (1, 4)))
    skeleton_index = draw_skeleton_index(jax.random.fold_in(seeds[6], 71), 0)
    near_ids = draw_near_ids(jax.random.fold_in(seeds[6], 71), 0)
    far_ids = draw_far_ids(jax.random.fold_in(seeds[6], 71), 0)
    return {"points": points, "charges": charges, "projection": projection, "skeleton_index": skeleton_index, "near_ids": near_ids, "far_ids": far_ids}


GAMMA = 1.0


def kernel_terms(targets, sources, weights):
    target_f32 = targets.astype(jnp.float32)
    source_f32 = sources.astype(jnp.float32)
    inner_terms = jnp.dot(targets.T, sources, preferred_element_type=jnp.float32)
    distance = jnp.sum(target_f32 * target_f32, axis=0)[:, None] + jnp.sum(source_f32 * source_f32, axis=0)[None, :] - 2.0 * inner_terms
    kernel = jnp.exp(-GAMMA * distance)
    return jnp.dot(weights.astype(jnp.float32), kernel.T, precision=lax.Precision.HIGHEST, preferred_element_type=jnp.float32)


def reference(points, charges, projection, skeleton_index, near_ids, far_ids):
    def skeleton_pair(leaf_pair):
        return jnp.dot(leaf_pair[0], leaf_pair[1].T, preferred_element_type=jnp.float32).astype(jnp.bfloat16)

    skeleton_charges = lax.map(skeleton_pair, (charges, projection))
    skeleton_points = jnp.take_along_axis(points, skeleton_index[:, None, :], axis=2)

    def per_leaf(target_item):
        targets, near_row, far_row = target_item
        near_points = points[near_row].transpose(1, 0, 2).reshape(DIM, NEAR * LEAF)
        far_points = skeleton_points[far_row].transpose(1, 0, 2).reshape(DIM, FAR * SKEL)
        near_weights = charges[near_row].transpose(1, 0, 2).reshape(RHS, NEAR * LEAF)
        far_weights = skeleton_charges[far_row].transpose(1, 0, 2).reshape(RHS, FAR * SKEL)
        sources = jnp.concatenate([near_points, far_points], axis=1)
        weights = jnp.concatenate([near_weights, far_weights], axis=1)
        return kernel_terms(targets, sources, weights)

    return lax.map(per_leaf, (points, near_ids, far_ids))
```

```python
import functools
import math

import jax
import jax.numpy as jnp
from jax import lax
from jax.experimental import pallas as pl
from jax.experimental.pallas import tpu as pltpu
from jax.sharding import PartitionSpec as P

MESH = pl.DeviceIdType.MESH
ANY = pl.BlockSpec(memory_space=pl.ANY)
VMEM = pl.BlockSpec(memory_space=pltpu.VMEM)
SMEM = pl.BlockSpec(memory_space=pltpu.SMEM)
RING = 4
NEAR_SLOTS = 6
FAR_SLOTS = 10
LIMIT = 62 * 1024 * 1000
F32 = jnp.float32
BF16 = jnp.bfloat16


def torus_position():
    leaf = lax.axis_index("leaf")
    chip = leaf // 2
    return chip // RING, chip % RING, leaf % 2, lax.axis_index("nbr")


def wrap(value):
    return lax.rem(value + 2 * RING, RING)


def pick(first_is_x, u, v):
    return u * RING + v if first_is_x else v * RING + u


def quarter_kernel(charges, projection, out):
    half = charges.shape[0] // 2

    def body(leaf, carry):
        parts = []
        for item in (leaf, leaf + half):
            parts.append(
                lax.dot_general(
                    charges[item], projection[item], (((1,), (1,)), ((), ())), preferred_element_type=F32
                )
            )
        out[leaf] = jnp.concatenate(parts, axis=1).astype(BF16)
        return carry

    lax.fori_loop(0, half, body, 0, unroll=2)


def gather_kernel(
    points, charges, quarter, index, ids,
    x_all, points_sib, charges_sib, index_sib, quarter_own, quarter_sib, ids_all,
    send_x, recv_x, send_s, recv_s, send_i, recv_i, local_sem,
):
    x, y, core, z = torus_position()
    n_z = quarter_own.shape[0]
    leaf_dev, dim, _ = points.shape
    cols = x_all.shape[3]
    half, part = leaf_dev // 2, leaf_dev // 4
    me = (x * RING + y) * n_z + z
    n_ids = ids_all.shape[0]

    def device(chip, core_at, z_at):
        return (chip * 2 + core_at, z_at)

    own_ids = pltpu.make_async_copy(ids, ids_all.at[me], local_sem)
    own_ids.start()

    def send_ids(step, carry):
        peer = lax.rem(me + step, n_ids)
        pltpu.make_async_remote_copy(
            src_ref=ids, dst_ref=ids_all.at[me], send_sem=send_i, recv_sem=recv_i,
            device_id=device(peer // n_z, core, lax.rem(peer, n_z)), device_id_type=MESH,
        ).start()
        return carry

    lax.fori_loop(1, n_ids, send_ids, 0)

    sends = []

    def message(kind, sems, src, dst, target):
        copy = pltpu.make_async_remote_copy(
            src_ref=src, dst_ref=dst, send_sem=sems[0].at[kind], recv_sem=sems[1].at[kind],
            device_id=target, device_id_type=MESH,
        )
        return copy

    def start(copy):
        copy.start()
        sends.append(copy)

    here = x * RING + y
    side = (send_s, recv_s)
    line = (send_x, recv_x)

    own_x = []
    for half_at in range(2):
        first_x = half_at == 0
        u, v = (x, y) if first_x else (y, x)
        base = half_at * half
        rows = pl.ds(base, half)
        src = points.at[rows, :, pl.ds(pl.multiple_of(z * cols, cols), cols)]
        dst = x_all.at[here, rows]
        kinds = 20 * half_at
        own_x.append(
            [
                message(kinds + 0, line, src, dst, device(pick(first_x, wrap(u + 1), v), core, z)),
                message(kinds + 1, line, src, dst, device(pick(first_x, wrap(u - 1), v), core, z)),
                message(kinds + 4, line, src, dst, device(pick(first_x, u, wrap(v + 1)), core, z)),
                message(kinds + 5, line, src, dst, device(pick(first_x, u, wrap(v - 1)), core, z)),
            ]
        )
    for at in range(4):
        for half_at in range(2):
            start(own_x[half_at][at])

    z_copies = []
    for step in range(1, n_z):
        copy = message(step, side, quarter, quarter_own.at[z], device(here, core, lax.rem(z + step, n_z)))
        start(copy)
        z_copies.append(copy)
    sib_copies = []
    for at, (src, dst) in enumerate(((points, points_sib), (charges, charges_sib), (index, index_sib))):
        copy = message(8 + at, side, src, dst, device(here, 1 - core, z))
        start(copy)
        sib_copies.append(copy)
    copy = message(0, side, quarter, quarter_sib.at[z], device(here, 1 - core, z))
    start(copy)
    sib_copies.append(copy)

    def item(half_at, du, dv, quarter_at=None):
        first_x = half_at == 0
        u, v = (x, y) if first_x else (y, x)
        rows = pl.ds(half_at * half, half) if quarter_at is None else pl.ds(half_at * half + quarter_at * part, part)
        return x_all.at[pick(first_x, wrap(u + du), wrap(v + dv)), rows]

    def target(half_at, du, dv):
        first_x = half_at == 0
        u, v = (x, y) if first_x else (y, x)
        return device(pick(first_x, wrap(u + du), wrap(v + dv)), core, z)

    def arrived(half_at, kind, ref):
        message(20 * half_at + kind, line, ref, ref, target(half_at, 1, 0)).wait_recv()

    def forward(half_at, kind, ref, du, dv):
        start(message(20 * half_at + kind, line, ref, ref, target(half_at, du, dv)))

    def across(half_at, slot, du):
        ref = item(half_at, du, 0)
        forward(half_at, 4 + 4 * slot, ref, 0, 1)
        forward(half_at, 5 + 4 * slot, ref, 0, -1)

    def relay(half_at, slot, du):
        arrived(half_at, 4 + 4 * slot, item(half_at, du, -1))
        forward(half_at, 6 + 4 * slot, item(half_at, du, -1, 0), 0, 1)
        arrived(half_at, 5 + 4 * slot, item(half_at, du, 1))
        forward(half_at, 7 + 4 * slot, item(half_at, du, 1, 1), 0, -1)

    for half_at in range(2):
        arrived(half_at, 0, item(half_at, -1, 0))
        forward(half_at, 2, item(half_at, -1, 0, 0), 1, 0)
        across(half_at, 1, -1)
    for half_at in range(2):
        arrived(half_at, 1, item(half_at, 1, 0))
        forward(half_at, 3, item(half_at, 1, 0, 1), -1, 0)
        across(half_at, 2, 1)
    for half_at in range(2):
        relay(half_at, 0, 0)
    for step in range(1, n_z):
        z_copies[step - 1].wait_recv()
        slot = lax.rem(z - step + n_z, n_z)
        ref = quarter_own.at[slot]
        copy = message(4 + step, side, ref, quarter_sib.at[slot], device(here, 1 - core, z))
        start(copy)
        sib_copies.append(copy)
    for half_at in range(2):
        arrived(half_at, 2, item(half_at, 2, 0, 0))
        arrived(half_at, 3, item(half_at, 2, 0, 1))
        across(half_at, 3, 2)
    for slot, du in ((1, -1), (2, 1), (3, 2)):
        for half_at in range(2):
            relay(half_at, slot, du)
    for slot, du in ((0, 0), (1, -1), (2, 1), (3, 2)):
        for half_at in range(2):
            arrived(half_at, 6 + 4 * slot, item(half_at, du, 2, 0))
            arrived(half_at, 7 + 4 * slot, item(half_at, du, 2, 1))
    for copy in sib_copies:
        copy.wait_recv()
    for copy in sends:
        copy.wait_send()
    own_ids.wait()
    others = ids_all.at[pl.ds(0, n_ids - 1)]
    every = pltpu.make_async_remote_copy(
        src_ref=others, dst_ref=others, send_sem=send_i, recv_sem=recv_i,
        device_id=target(0, 1, 0), device_id_type=MESH,
    )
    every.wait_send()
    every.wait_recv()


def table_kernel(leaf_dev, near_dev, far_dev, n_z, ids_all, table):
    x, y, core, _ = torus_position()
    chip = x * RING + y
    rows = ids_all.shape[0]
    lane = lax.broadcasted_iota(jnp.int32, (rows, 128), 1)
    row = lax.broadcasted_iota(jnp.int32, (rows, 128), 0)
    upper = lax.broadcasted_iota(jnp.int32, (128, 128), 0) <= lax.broadcasted_iota(jnp.int32, (128, 128), 1)
    upper = jnp.where(upper, 1.0, 0.0).astype(BF16)
    result = jnp.zeros((rows, 128), jnp.int32)
    for at, (per_leaf, slots, start) in enumerate(((near_dev, NEAR_SLOTS, 0), (far_dev, FAR_SLOTS, NEAR_SLOTS))):
        ids = ids_all[:, at, :]
        named = lax.div(ids, 2 * leaf_dev)
        member = jnp.logical_and(named == chip, ids >= 0)
        source = lax.rem(lax.rem(ids, 2 * leaf_dev) + core * leaf_dev, 2 * leaf_dev)
        code = (lax.div(row, n_z) * leaf_dev + lax.div(lane, per_leaf)) * (2 * leaf_dev) + source
        flags = jnp.where(member, 1.0, 0.0)
        upto = jnp.dot(flags.astype(BF16), upper, preferred_element_type=F32).astype(jnp.int32)
        for slot in range(slots):
            chosen = jnp.logical_and(member, upto == slot + 1)
            value = jnp.sum(jnp.where(chosen, code, 0), axis=1, keepdims=True)
            result = jnp.where(lane == start + slot, value, result)
        count = jnp.sum(jnp.where(member, 1, 0), axis=1, keepdims=True)
        result = jnp.where(lane == NEAR_SLOTS + FAR_SLOTS + at, count, result)
    table[...] = result


def norm_rows(coords, sign_first):
    values = coords.astype(F32)
    norm = -jnp.sum(values * values, axis=0, keepdims=True)
    high = norm.astype(BF16).astype(F32)
    rest = norm - high
    middle = rest.astype(BF16).astype(F32)
    low = rest - middle
    shape = (16, coords.shape[1])
    row = lax.broadcasted_iota(jnp.int32, shape, 0)
    start = 0 if sign_first else 3
    ones = 3 if sign_first else 0
    result = jnp.where(jnp.logical_and(row >= ones, row < ones + 3), 1.0, 0.0)
    for at, piece in enumerate((high, middle, low)):
        result = jnp.where(row == start + at, jnp.broadcast_to(piece, shape), result)
    return result.astype(BF16)


def pair_kernel(
    table, x_all, points, charges, quarter, index, points_sib, charges_sib, index_sib, quarter_own, quarter_sib,
    out,
    x_raw, x_aug, y_table, w_table, p_buf, i_buf, q_buf, acc, s_a, s_b, items, sems,
):
    x, y, core, z = torus_position()
    chips, leaf_dev, dim, cols = x_all.shape
    leaf = points.shape[2]
    skel = index.shape[1]
    n_z = quarter_own.shape[0]
    here = x * RING + y
    sources = 2 * leaf_dev
    targets = chips * leaf_dev
    hold = leaf_dev // 2
    piece = skel // n_z

    loads = []

    def load(at, src, dst):
        copy = pltpu.make_async_copy(src, dst, sems.at[at])
        copy.start()
        loads.append(copy)

    load(0, points, p_buf.at[0])
    load(1, points_sib, p_buf.at[1])
    load(2, index, i_buf.at[0])
    load(3, index_sib, i_buf.at[1])
    load(4, quarter_own, q_buf.at[0])
    load(5, quarter_sib, q_buf.at[1])
    load(6, x_all, x_raw)
    at = 8
    for side, ref in ((0, charges), (1, charges_sib)):
        for half in range(2):
            load(
                at, ref.at[:, :, pl.ds(half * skel, skel)],
                w_table.at[pl.ds(half * sources + side * leaf_dev, leaf_dev)],
            )
            at += 1

    rows = table.shape[0]
    span = 3 * sources

    def fill(row, count):
        for slot in range(NEAR_SLOTS):
            code = table[row, slot]
            base = lax.div(code, sources) * 256 + lax.rem(code, sources)
            items[count + 2 * slot] = base
            items[count + 2 * slot + 1] = base + sources
        count = count + 2 * table[row, NEAR_SLOTS + FAR_SLOTS]
        for slot in range(FAR_SLOTS):
            code = table[row, NEAR_SLOTS + slot]
            items[count + slot] = lax.div(code, sources) * 256 + lax.rem(code, sources) + 2 * sources
        return count + table[row, NEAR_SLOTS + FAR_SLOTS + 1]

    count = lax.fori_loop(0, rows, fill, 0)
    for at in range(12):
        items[count + at] = targets * 256

    for copy in loads:
        copy.wait()
    copy = pltpu.make_async_copy(quarter, q_buf.at[0, z], sems.at[7])
    copy.start()
    own = pltpu.make_async_copy(
        points.at[:, :, pl.ds(pl.multiple_of(z * cols, cols), cols)], x_raw.at[here], sems.at[6]
    )
    own.start()

    def zero(at, carry):
        acc[at] = jnp.zeros(acc.shape[1:], F32)
        return carry

    lax.fori_loop(0, targets + 1, zero, 0, unroll=4)
    copy.wait()
    own.wait()

    pad = jnp.zeros((16, cols), BF16)

    def widen(at, carry):
        coords = x_raw[lax.div(at, leaf_dev), lax.rem(at, leaf_dev)]
        x_aug[at] = jnp.concatenate([coords, norm_rows(coords, True), pad], axis=0)
        return carry

    lax.fori_loop(0, targets, widen, 0, unroll=4)

    wide_pad = jnp.zeros((16, leaf), BF16)
    point_number = lax.broadcasted_iota(jnp.int32, (leaf, skel), 0)

    def source(at, carry):
        side, item = lax.div(at, leaf_dev), lax.rem(at, leaf_dev)
        coords = p_buf[side, item]
        block = jnp.concatenate([coords + coords, norm_rows(coords, False), wide_pad], axis=0)
        block = jnp.concatenate([block, block], axis=0)
        turned = block.T
        y_table[at] = turned[:skel]
        y_table[sources + at] = turned[skel:]
        chosen = point_number == i_buf[side, pl.ds(item, 1), :]
        chosen = jnp.where(chosen, 1.0, 0.0).astype(BF16)
        picked = jnp.dot(block, chosen, preferred_element_type=F32).astype(BF16)
        y_table[2 * sources + at] = picked.T
        return carry

    lax.fori_loop(0, sources, source, 0, unroll=2)

    def assemble(at, carry):
        side, item = lax.div(at, hold), lax.rem(at, hold)
        chunks = [q_buf[side, step, item] for step in range(n_z)]
        for half in range(2):
            pieces = [chunk[:, half * piece : (half + 1) * piece] for chunk in chunks]
            w_table[2 * sources + side * leaf_dev + half * hold + item] = jnp.concatenate(pieces, axis=1)
        return carry

    lax.fori_loop(0, 2 * hold, assemble, 0, unroll=2)

    empty = jnp.zeros((64, cols), BF16)
    low_lanes = lax.broadcasted_iota(jnp.int32, (skel, 128), 1) < 64

    def read(at):
        code = items[at]
        return lax.div(code, 256), lax.rem(code, 256)

    def scores(group, buf):
        for duo in range(2):
            t_0, u_0 = read(group * 4 + 2 * duo)
            t_1, u_1 = read(group * 4 + 2 * duo + 1)
            x_0 = x_aug[jnp.minimum(t_0, targets - 1)]
            x_1 = x_aug[jnp.minimum(t_1, targets - 1)]
            right = jnp.concatenate(
                [jnp.concatenate([x_0, empty], axis=0), jnp.concatenate([empty, x_1], axis=0)], axis=1
            )
            left = jnp.where(low_lanes, y_table[u_0], y_table[u_1])
            buf[duo] = jnp.dot(left, right, preferred_element_type=F32)

    def sums(group, buf):
        for duo in range(2):
            t_0, u_0 = read(group * 4 + 2 * duo)
            t_1, u_1 = read(group * 4 + 2 * duo + 1)
            kernel = jnp.exp(buf[duo]).astype(BF16)
            weights = jnp.concatenate([w_table[u_0], w_table[u_1]], axis=0)
            terms = jnp.dot(weights, kernel, preferred_element_type=F32)
            rhs = terms.shape[0] // 2
            acc[t_0] = acc[t_0] + terms[:rhs, :cols]
            acc[t_1] = acc[t_1] + terms[rhs:, cols:]

    scores(0, s_a)

    def step(at, carry):
        scores(2 * at + 1, s_b)
        sums(2 * at, s_a)
        scores(2 * at + 2, s_a)
        sums(2 * at + 1, s_b)
        return carry

    lax.fori_loop(0, lax.div(count + 7, 8), step, 0)
    done = pltpu.make_async_copy(acc.at[pl.ds(0, targets)], out, sems.at[0])
    done.start()
    done.wait()


def reduce_kernel(
    part_all, out, held, send_8, recv_8, send_16, recv_16, scale_s8, scale_r8, scale_s16, scale_r16,
    load_sems, sem_s8, sem_r8, sem_s16, sem_r16,
):
    x, y, core, z = torus_position()
    leaf_dev = part_all.shape[1]
    half, part = leaf_dev // 2, leaf_dev // 4
    order = ((2, 0), (1, 1), (-1, 2), (0, 3))

    def chip_at(half_at, du, dv):
        first_x = half_at == 0
        u, v = (x, y) if first_x else (y, x)
        return pick(first_x, wrap(u + du), wrap(v + dv))

    loads = {}
    for du, _ in order:
        for dv, _ in order:
            for half_at in range(2):
                slot = chip_at(half_at, du, dv)
                ref = pl.ds(half_at * half, half)
                copy = pltpu.make_async_copy(
                    part_all.at[slot, ref], held.at[slot, ref], load_sems.at[len(loads)]
                )
                copy.start()
                loads[half_at, du, dv] = copy

    sends = []

    def wires(size, kind, chip):
        big = size == half
        pairs = (
            ((send_16, recv_16, sem_s16, sem_r16, 0), (scale_s16, scale_r16, sem_s16, sem_r16, 1))
            if big
            else ((send_8, recv_8, sem_s8, sem_r8, 0), (scale_s8, scale_r8, sem_s8, sem_r8, 1))
        )
        return [
            pltpu.make_async_remote_copy(
                src_ref=src.at[kind], dst_ref=dst.at[kind], send_sem=s.at[2 * kind + at], recv_sem=r.at[2 * kind + at],
                device_id=(chip * 2 + core, z), device_id_type=MESH,
            )
            for src, dst, s, r, at in pairs
        ]

    def unpack(size, kind, row):
        data, scale = (recv_16, scale_r16) if size == half else (recv_8, scale_r8)
        return data[kind, row].astype(jnp.int32).astype(F32) * scale[kind, pl.ds(row, 1), :]

    def send(size, kind, chip, value_at):
        data, scale = (send_16, scale_s16) if size == half else (send_8, scale_s8)

        def body(row, carry):
            value = value_at(row)
            top = jnp.maximum(jnp.max(jnp.abs(value), axis=0, keepdims=True), 1e-30)
            scale[kind, pl.ds(row, 1), :] = top * (1.0 / 32767.0)
            data[kind, row] = jnp.round(value * (32767.0 / top)).astype(jnp.int32).astype(jnp.int16)
            return carry

        lax.fori_loop(0, size, body, 0, unroll=2)
        for copy in wires(size, kind, chip):
            copy.start()
            sends.append(copy)

    def wait(size, kind):
        for copy in wires(size, kind, chip_at(0, 1, 0)):
            copy.wait_recv()

    def ready(half_at, du, dv):
        loads.pop((half_at, du, dv)).wait()

    for dv, at in order:
        for half_at in range(2):
            base = half_at * half
            ready(half_at, 2, dv)
            slot = chip_at(half_at, 2, dv)
            kind = half_at * 10 + 2 * at
            send(part, kind, chip_at(half_at, 1, 0), lambda row: held[slot, base + row])
            send(part, kind + 1, chip_at(half_at, -1, 0), lambda row: held[slot, base + part + row])
    for dv, at in order:
        for half_at in range(2):
            base = half_at * half
            for du, side in ((1, 0), (-1, 1)):
                ready(half_at, du, dv)
                slot = chip_at(half_at, du, dv)
                kind = half_at * 10 + 2 * at + side
                wait(part, kind)

                def add(row, carry):
                    spot = base + side * part + row
                    held[slot, spot] = held[slot, spot] + unpack(part, kind, row)
                    return carry

                lax.fori_loop(0, part, add, 0, unroll=2)
                send(half, kind, chip_at(half_at, du, 0), lambda row: held[slot, base + row])
    for dv, at in order:
        for half_at in range(2):
            base = half_at * half
            ready(half_at, 0, dv)
            slot = chip_at(half_at, 0, dv)
            kind = half_at * 10 + 2 * at
            wait(half, kind)
            wait(half, kind + 1)

            def keep(row, carry):
                held[slot, base + row] = held[slot, base + row] + unpack(half, kind, row) + unpack(half, kind + 1, row)
                return carry

            lax.fori_loop(0, half, keep, 0, unroll=2)
            if dv == 2:
                for sign, side in ((1, 0), (-1, 1)):
                    send(
                        part, half_at * 10 + 8 + side, chip_at(half_at, 0, sign),
                        lambda row: held[slot, base + side * part + row],
                    )
            elif dv != 0:
                side = 0 if dv == 1 else 1
                late = half_at * 10 + 8 + side
                wait(part, late)

                def add_late(row, carry):
                    spot = base + side * part + row
                    held[slot, spot] = held[slot, spot] + unpack(part, late, row)
                    return carry

                lax.fori_loop(0, part, add_late, 0, unroll=2)
                send(half, late, chip_at(half_at, 0, dv), lambda row: held[slot, base + row])
    for half_at in range(2):
        base = half_at * half
        slot = chip_at(half_at, 0, 0)
        kind = half_at * 10 + 8
        wait(half, kind)
        wait(half, kind + 1)

        def finish(row, carry):
            out[base + row] = held[slot, base + row] + unpack(half, kind, row) + unpack(half, kind + 1, row)
            return carry

        lax.fori_loop(0, half, finish, 0, unroll=2)
    for copy in sends:
        copy.wait_send()


def per_device(points, charges, projection, skeleton_index, near_ids, far_ids):
    leaf_dev, dim, leaf = points.shape
    rhs = charges.shape[1]
    skel = skeleton_index.shape[1]
    n_z = lax.axis_size("nbr")
    chips = lax.axis_size("leaf") // 2
    cols = leaf // n_z
    near_dev, far_dev = near_ids.shape[1], far_ids.shape[1]
    sources, targets = 2 * leaf_dev, chips * leaf_dev
    params = functools.partial(pltpu.CompilerParams, vmem_limit_bytes=LIMIT)
    dma = pltpu.SemaphoreType.DMA
    shape = jax.ShapeDtypeStruct

    def row_of(ids):
        flat = ids.reshape(1, -1)
        return jnp.pad(flat, ((0, 0), (0, 128 - flat.shape[1])), constant_values=-1)

    ids = jnp.concatenate([row_of(near_ids), row_of(far_ids), jnp.full((6, 128), -1, jnp.int32)], axis=0)

    quarter = pl.pallas_call(
        quarter_kernel,
        out_shape=shape((leaf_dev // 2, rhs, 2 * skel // n_z), BF16),
        in_specs=[VMEM, VMEM],
        out_specs=VMEM,
        name="quarter",
        compiler_params=params(),
    )(charges, projection)
    x_all, points_sib, charges_sib, index_sib, quarter_own, quarter_sib, ids_all = pl.pallas_call(
        gather_kernel,
        out_shape=[
            shape((chips, leaf_dev, dim, cols), BF16),
            shape(points.shape, BF16),
            shape(charges.shape, BF16),
            shape(skeleton_index.shape, jnp.int32),
            shape((n_z,) + quarter.shape, BF16),
            shape((n_z,) + quarter.shape, BF16),
            shape((chips * n_z, 8, 128), jnp.int32),
        ],
        in_specs=[ANY] * 5,
        out_specs=[ANY] * 7,
        scratch_shapes=[dma((40,)), dma((40,)), dma((12,)), dma((12,)), dma, dma, dma],
        name="gather",
        compiler_params=params(has_side_effects=True),
    )(points, charges, quarter, skeleton_index, ids)
    table = pl.pallas_call(
        functools.partial(table_kernel, leaf_dev, near_dev, far_dev, n_z),
        out_shape=shape((chips * n_z, 128), jnp.int32),
        in_specs=[VMEM],
        out_specs=VMEM,
        name="table",
        compiler_params=params(),
    )(ids_all)
    partial_sums = pl.pallas_call(
        pair_kernel,
        out_shape=shape((targets, rhs, cols), F32),
        in_specs=[SMEM] + [ANY] * 10,
        out_specs=ANY,
        scratch_shapes=[
            pltpu.VMEM((chips, leaf_dev, dim, cols), BF16),
            pltpu.VMEM((targets, 64, cols), BF16),
            pltpu.VMEM((3 * sources, skel, 128), BF16),
            pltpu.VMEM((3 * sources, rhs, skel), BF16),
            pltpu.VMEM((2,) + points.shape, BF16),
            pltpu.VMEM((2,) + skeleton_index.shape, jnp.int32),
            pltpu.VMEM((2, n_z) + quarter.shape, BF16),
            pltpu.VMEM((targets + 1, rhs, cols), F32),
            pltpu.VMEM((2, skel, 2 * cols), F32),
            pltpu.VMEM((2, skel, 2 * cols), F32),
            pltpu.SMEM((chips * n_z * (2 * NEAR_SLOTS + FAR_SLOTS) + 32,), jnp.int32),
            dma((16,)),
        ],
        name="pairs",
        compiler_params=params(),
    )(
        table, x_all, points, charges, quarter, skeleton_index, points_sib, charges_sib, index_sib, quarter_own,
        quarter_sib,
    )
    half, part = leaf_dev // 2, leaf_dev // 4
    return pl.pallas_call(
        reduce_kernel,
        out_shape=shape((leaf_dev, rhs, cols), F32),
        in_specs=[ANY],
        out_specs=VMEM,
        scratch_shapes=[
            pltpu.VMEM((chips, leaf_dev, rhs, cols), F32),
            pltpu.VMEM((20, part, rhs, cols), jnp.int16),
            pltpu.VMEM((20, part, rhs, cols), jnp.int16),
            pltpu.VMEM((20, half, rhs, cols), jnp.int16),
            pltpu.VMEM((20, half, rhs, cols), jnp.int16),
            pltpu.VMEM((20, part, cols), F32),
            pltpu.VMEM((20, part, cols), F32),
            pltpu.VMEM((20, half, cols), F32),
            pltpu.VMEM((20, half, cols), F32),
            dma((32,)), dma((40,)), dma((40,)), dma((40,)), dma((40,)),
        ],
        name="reduce",
        compiler_params=params(has_side_effects=True),
    )(partial_sums.reshape(chips, leaf_dev, rhs, cols))


def solution(mesh):
    in_specs = (
        P("leaf", None, None),
        P("leaf", None, None),
        P("leaf", "nbr", None),
        P("leaf", None),
        P("leaf", "nbr"),
        P("leaf", "nbr"),
    )
    out_specs = P("leaf", None, "nbr")
    return jax.shard_map(per_device, mesh=mesh, in_specs=in_specs, out_specs=out_specs, check_vma=False)
```

```python
import functools
import math

import jax
import jax.numpy as jnp
from jax import lax
from jax.experimental import pallas as pl
from jax.experimental.pallas import tpu as pltpu
from jax.sharding import PartitionSpec as P

MESH = pl.DeviceIdType.MESH
ANY = pl.BlockSpec(memory_space=pl.ANY)
VMEM = pl.BlockSpec(memory_space=pltpu.VMEM)
SMEM = pl.BlockSpec(memory_space=pltpu.SMEM)
RING = 4
NEAR_SLOTS = 6
FAR_SLOTS = 10
DUOS = 6
LIMIT = 62 * 1024 * 1000
F32 = jnp.float32
BF16 = jnp.bfloat16


def torus_position():
    leaf = lax.axis_index("leaf")
    chip = leaf // 2
    return chip // RING, chip % RING, leaf % 2, lax.axis_index("nbr")


def wrap(value):
    return lax.rem(value + 2 * RING, RING)


def pick(first_is_x, u, v):
    return u * RING + v if first_is_x else v * RING + u


def gather_kernel(
    points, charges, projection, index, ids,
    y_out, x_out, w_out, charges_sib, ids_all,
    p_buf, i_buf, c_buf, j_buf, q_buf, x_raw, y_table, x_aug, w_skel,
    send_x, recv_x, send_s, recv_s, send_i, recv_i, load_sems, out_sems,
):
    x, y, core, z = torus_position()
    n_z = q_buf.shape[1]
    leaf_dev, dim, leaf = points.shape
    skel = index.shape[1]
    cols = x_raw.shape[3]
    half, part = leaf_dev // 2, leaf_dev // 4
    hold = leaf_dev // 2
    piece = skel // n_z
    me = (x * RING + y) * n_z + z
    n_ids = ids_all.shape[0]
    here = x * RING + y
    own_cols = pl.ds(pl.multiple_of(z * cols, cols), cols)

    def device(chip, core_at, z_at):
        return (chip * 2 + core_at, z_at)

    sends = []

    def message(kind, sems, src, dst, target):
        return pltpu.make_async_remote_copy(
            src_ref=src, dst_ref=dst, send_sem=sems[0].at[kind], recv_sem=sems[1].at[kind],
            device_id=target, device_id_type=MESH,
        )

    def start(copy):
        copy.start()
        sends.append(copy)

    side = (send_s, recv_s)
    line = (send_x, recv_x)

    own_x = []
    for half_at in range(2):
        first_x = half_at == 0
        u, v = (x, y) if first_x else (y, x)
        rows = pl.ds(half_at * half, half)
        src = points.at[rows, :, own_cols]
        dst = x_raw.at[here, rows]
        kinds = 20 * half_at
        own_x.append(
            [
                message(kinds + 0, line, src, dst, device(pick(first_x, wrap(u + 1), v), core, z)),
                message(kinds + 1, line, src, dst, device(pick(first_x, wrap(u - 1), v), core, z)),
                message(kinds + 4, line, src, dst, device(pick(first_x, u, wrap(v + 1)), core, z)),
                message(kinds + 5, line, src, dst, device(pick(first_x, u, wrap(v - 1)), core, z)),
            ]
        )
    for at in range(4):
        for half_at in range(2):
            start(own_x[half_at][at])

    loads = []
    for at, (src, dst) in enumerate(
        (
            (charges, c_buf),
            (projection, j_buf),
            (points, p_buf.at[0]),
            (index, i_buf.at[0]),
            (points.at[:, :, own_cols], x_raw.at[here]),
            (ids, ids_all.at[me]),
        )
    ):
        copy = pltpu.make_async_copy(src, dst, load_sems.at[at])
        copy.start()
        loads.append(copy)

    sib_copies = []
    for at, (src, dst) in enumerate(((points, p_buf.at[1]), (index, i_buf.at[1]), (charges, charges_sib))):
        copy = message(8 + at, side, src, dst, device(here, 1 - core, z))
        start(copy)
        sib_copies.append(copy)

    def send_ids(step, carry):
        peer = lax.rem(me + step, n_ids)
        pltpu.make_async_remote_copy(
            src_ref=ids, dst_ref=ids_all.at[me], send_sem=send_i, recv_sem=recv_i,
            device_id=device(peer // n_z, core, lax.rem(peer, n_z)), device_id_type=MESH,
        ).start()
        return carry

    lax.fori_loop(1, n_ids, send_ids, 0)

    loads[0].wait()
    loads[1].wait()

    def charge(item, carry):
        parts = []
        for at in (item, item + hold):
            parts.append(
                lax.dot_general(c_buf[at], j_buf[at], (((1,), (1,)), ((), ())), preferred_element_type=F32)
            )
        q_buf[0, z, item] = jnp.concatenate(parts, axis=1).astype(BF16)
        return carry

    lax.fori_loop(0, hold, charge, 0, unroll=2)
    z_copies = []
    own_quarter = q_buf.at[0, z]
    for step in range(1, n_z):
        copy = message(step, side, own_quarter, own_quarter, device(here, core, lax.rem(z + step, n_z)))
        start(copy)
        z_copies.append(copy)
    copy = message(0, side, own_quarter, q_buf.at[1, z], device(here, 1 - core, z))
    start(copy)
    sib_quarters = [copy]

    def item(half_at, du, dv, quarter_at=None):
        first_x = half_at == 0
        u, v = (x, y) if first_x else (y, x)
        rows = pl.ds(half_at * half, half) if quarter_at is None else pl.ds(half_at * half + quarter_at * part, part)
        return x_raw.at[pick(first_x, wrap(u + du), wrap(v + dv)), rows]

    def target(half_at, du, dv):
        first_x = half_at == 0
        u, v = (x, y) if first_x else (y, x)
        return device(pick(first_x, wrap(u + du), wrap(v + dv)), core, z)

    def arrived(half_at, kind, ref):
        message(20 * half_at + kind, line, ref, ref, target(half_at, 1, 0)).wait_recv()

    def forward(half_at, kind, ref, du, dv):
        start(message(20 * half_at + kind, line, ref, ref, target(half_at, du, dv)))

    def across(half_at, slot, du):
        ref = item(half_at, du, 0)
        forward(half_at, 4 + 4 * slot, ref, 0, 1)
        forward(half_at, 5 + 4 * slot, ref, 0, -1)

    def relay(half_at, slot, du):
        arrived(half_at, 4 + 4 * slot, item(half_at, du, -1))
        forward(half_at, 6 + 4 * slot, item(half_at, du, -1, 0), 0, 1)
        arrived(half_at, 5 + 4 * slot, item(half_at, du, 1))
        forward(half_at, 7 + 4 * slot, item(half_at, du, 1, 1), 0, -1)

    pad = jnp.zeros((16, cols), BF16)

    def widen(half_at, du, dv):
        first_x = half_at == 0
        u, v = (x, y) if first_x else (y, x)
        chip = pick(first_x, wrap(u + du), wrap(v + dv))
        base = half_at * half

        def body(at, carry):
            coords = x_raw[chip, base + at]
            x_aug[chip, base + at] = jnp.concatenate([coords, norm_rows(coords, True), pad], axis=0)
            return carry

        lax.fori_loop(0, half, body, 0, unroll=4)

    wide_pad = jnp.zeros((16, leaf), BF16)
    point_number = lax.broadcasted_iota(jnp.int32, (leaf, skel), 0)
    sources = 2 * leaf_dev

    def source(at_side, first, count):
        def body(at, carry):
            coords = p_buf[at_side, at]
            block = jnp.concatenate([coords + coords, norm_rows(coords, False), wide_pad], axis=0)
            block = jnp.concatenate([block, block], axis=0)
            turned = block.T
            row = at_side * leaf_dev + at
            y_table[row] = turned[:skel]
            y_table[sources + row] = turned[skel:]
            chosen = point_number == i_buf[at_side, pl.ds(at, 1), :]
            chosen = jnp.where(chosen, 1.0, 0.0).astype(BF16)
            picked = jnp.dot(block, chosen, preferred_element_type=F32).astype(BF16)
            y_table[2 * sources + row] = picked.T
            return carry

        lax.fori_loop(first, first + count, body, 0, unroll=2)

    outs = []

    def put(src, dst):
        copy = pltpu.make_async_copy(src, dst, out_sems.at[len(outs)])
        copy.start()
        outs.append(copy)

    def put_y(at_side):
        for block in range(3):
            rows = pl.ds(block * sources + at_side * leaf_dev, leaf_dev)
            put(y_table.at[rows], y_out.at[rows])

    def assemble(at_side):
        def body(at, carry):
            chunks = [q_buf[at_side, step, at] for step in range(n_z)]
            for half_at in range(2):
                pieces = [chunk[:, half_at * piece : (half_at + 1) * piece] for chunk in chunks]
                w_skel[at_side * leaf_dev + half_at * hold + at] = jnp.concatenate(pieces, axis=1)
            return carry

        lax.fori_loop(0, hold, body, 0, unroll=2)

    for half_at in range(2):
        arrived(half_at, 0, item(half_at, -1, 0))
        forward(half_at, 2, item(half_at, -1, 0, 0), 1, 0)
        across(half_at, 1, -1)
    for half_at in range(2):
        arrived(half_at, 1, item(half_at, 1, 0))
        forward(half_at, 3, item(half_at, 1, 0, 1), -1, 0)
        across(half_at, 2, 1)
    for half_at in range(2):
        relay(half_at, 0, 0)
    loads[2].wait()
    loads[3].wait()
    loads[4].wait()
    source(0, 0, leaf_dev // 2)
    for half_at in range(2):
        arrived(half_at, 2, item(half_at, 2, 0, 0))
        arrived(half_at, 3, item(half_at, 2, 0, 1))
        across(half_at, 3, 2)
    for step in range(1, n_z):
        z_copies[step - 1].wait_recv()
        slot = lax.rem(z - step + n_z, n_z)
        copy = message(4 + step, side, q_buf.at[0, slot], q_buf.at[1, slot], device(here, 1 - core, z))
        start(copy)
        sib_quarters.append(copy)
    source(0, leaf_dev // 2, leaf_dev // 2)
    put_y(0)
    for half_at in range(2):
        relay(half_at, 1, -1)
    sib_copies[0].wait_recv()
    sib_copies[1].wait_recv()
    source(1, 0, leaf_dev // 2)
    for half_at in range(2):
        relay(half_at, 2, 1)
    source(1, leaf_dev // 2, leaf_dev // 2)
    put_y(1)
    for half_at in range(2):
        for du in (0, -1, 1, 2):
            widen(half_at, du, 0)
    for half_at in range(2):
        relay(half_at, 3, 2)
    assemble(0)
    for copy in sib_quarters:
        copy.wait_recv()
    assemble(1)
    put(w_skel, w_out)
    for half_at in range(2):
        for dv in (-1, 1):
            for du in (0, -1, 1, 2):
                widen(half_at, du, dv)
    for slot, du in ((0, 0), (1, -1), (2, 1), (3, 2)):
        for half_at in range(2):
            arrived(half_at, 6 + 4 * slot, item(half_at, du, 2, 0))
            arrived(half_at, 7 + 4 * slot, item(half_at, du, 2, 1))
            widen(half_at, du, 2)
    put(x_aug, x_out)
    sib_copies[2].wait_recv()
    for copy in sends:
        copy.wait_send()
    loads[5].wait()
    others = ids_all.at[pl.ds(0, n_ids - 1)]
    every = pltpu.make_async_remote_copy(
        src_ref=others, dst_ref=others, send_sem=send_i, recv_sem=recv_i,
        device_id=target(0, 1, 0), device_id_type=MESH,
    )
    every.wait_send()
    every.wait_recv()
    for copy in outs:
        copy.wait()


def table_kernel(leaf_dev, near_dev, far_dev, n_z, ids_all, table):
    x, y, core, _ = torus_position()
    chip = x * RING + y
    rows = ids_all.shape[0]
    lane = lax.broadcasted_iota(jnp.int32, (rows, 128), 1)
    row = lax.broadcasted_iota(jnp.int32, (rows, 128), 0)
    upper = lax.broadcasted_iota(jnp.int32, (128, 128), 0) <= lax.broadcasted_iota(jnp.int32, (128, 128), 1)
    upper = jnp.where(upper, 1.0, 0.0).astype(BF16)
    result = jnp.zeros((rows, 128), jnp.int32)
    for at, (per_leaf, slots, start) in enumerate(((near_dev, NEAR_SLOTS, 0), (far_dev, FAR_SLOTS, NEAR_SLOTS))):
        ids = ids_all[:, at, :]
        named = lax.div(ids, 2 * leaf_dev)
        member = jnp.logical_and(named == chip, ids >= 0)
        source = lax.rem(lax.rem(ids, 2 * leaf_dev) + core * leaf_dev, 2 * leaf_dev)
        code = (lax.div(row, n_z) * leaf_dev + lax.div(lane, per_leaf)) * 256 + source + at * 4 * leaf_dev
        flags = jnp.where(member, 1.0, 0.0)
        upto = jnp.dot(flags.astype(BF16), upper, preferred_element_type=F32).astype(jnp.int32)
        for slot in range(slots):
            chosen = jnp.logical_and(member, upto == slot + 1)
            value = jnp.sum(jnp.where(chosen, code, 0), axis=1, keepdims=True)
            result = jnp.where(lane == start + slot, value, result)
        count = jnp.sum(jnp.where(member, 1, 0), axis=1, keepdims=True)
        result = jnp.where(lane == NEAR_SLOTS + FAR_SLOTS + at, count, result)
    table[...] = result


def norm_rows(coords, sign_first):
    values = coords.astype(F32)
    norm = -jnp.sum(values * values, axis=0, keepdims=True)
    high = norm.astype(BF16).astype(F32)
    rest = norm - high
    middle = rest.astype(BF16).astype(F32)
    low = rest - middle
    shape = (16, coords.shape[1])
    row = lax.broadcasted_iota(jnp.int32, shape, 0)
    start = 0 if sign_first else 3
    ones = 3 if sign_first else 0
    result = jnp.where(jnp.logical_and(row >= ones, row < ones + 3), 1.0, 0.0)
    for at, piece in enumerate((high, middle, low)):
        result = jnp.where(row == start + at, jnp.broadcast_to(piece, shape), result)
    return result.astype(BF16)


def pair_kernel(
    table, y_in, x_in, w_in, charges, charges_sib,
    out,
    x_aug, y_table, w_table, acc, s_a, s_b, items, ends, sems, out_sem,
):
    leaf_dev, rhs, _ = charges.shape
    skel = y_in.shape[1]
    targets, _, cols = x_in.shape
    n_z = table.shape[0] // (targets // leaf_dev)
    sources = 2 * leaf_dev

    loads = []

    def load(src, dst):
        copy = pltpu.make_async_copy(src, dst, sems.at[len(loads)])
        copy.start()
        loads.append(copy)

    load(x_in, x_aug)
    load(y_in, y_table)
    load(w_in, w_table.at[pl.ds(2 * sources, sources)])
    for side, ref in ((0, charges), (1, charges_sib)):
        for half in range(2):
            load(
                ref.at[:, :, pl.ds(half * skel, skel)],
                w_table.at[pl.ds(half * sources + side * leaf_dev, leaf_dev)],
            )

    def fill(chip, count):
        for step in range(n_z):
            row = chip * n_z + step
            for slot in range(NEAR_SLOTS):
                code = table[row, slot]
                items[count + 2 * slot] = code
                items[count + 2 * slot + 1] = code + sources
            count = count + 2 * table[row, NEAR_SLOTS + FAR_SLOTS]
            for slot in range(FAR_SLOTS):
                items[count + slot] = table[row, NEAR_SLOTS + slot]
            count = count + table[row, NEAR_SLOTS + FAR_SLOTS + 1]
        ends[chip] = count
        return count

    chips = table.shape[0] // n_z
    count = lax.fori_loop(0, chips, fill, 0)
    for at in range(6 * DUOS):
        items[count + at] = targets * 256

    def zero(at, carry):
        acc[at] = jnp.zeros(acc.shape[1:], F32)
        return carry

    lax.fori_loop(0, targets + 1, zero, 0, unroll=4)
    for copy in loads:
        copy.wait()

    empty = jnp.zeros((64, cols), BF16)
    low_lanes = lax.broadcasted_iota(jnp.int32, (skel, 128), 1) < 64

    def read(at):
        code = items[at]
        return lax.shift_right_logical(code, 8), jnp.bitwise_and(code, 255)

    def scores(group, buf, at):
        for duo in [at]:
            t_0, u_0 = read(group * 2 * DUOS + 2 * duo)
            t_1, u_1 = read(group * 2 * DUOS + 2 * duo + 1)
            x_0 = x_aug[jnp.minimum(t_0, targets - 1)]
            x_1 = x_aug[jnp.minimum(t_1, targets - 1)]
            right = jnp.concatenate(
                [jnp.concatenate([x_0, empty], axis=0), jnp.concatenate([empty, x_1], axis=0)], axis=1
            )
            left = jnp.where(low_lanes, y_table[u_0], y_table[u_1])
            buf[duo] = jnp.dot(left, right, preferred_element_type=F32)

    def sums(group, buf, at):
        for duo in [at]:
            t_0, u_0 = read(group * 2 * DUOS + 2 * duo)
            t_1, u_1 = read(group * 2 * DUOS + 2 * duo + 1)
            kernel = jnp.exp(buf[duo]).astype(BF16)
            weights = jnp.concatenate([w_table[u_0], w_table[u_1]], axis=0)
            terms = jnp.dot(weights, kernel, preferred_element_type=F32)
            rhs = terms.shape[0] // 2
            acc[t_0] = acc[t_0] + terms[:rhs, :cols]
            acc[t_1] = acc[t_1] + terms[rhs:, cols:]

    for duo in range(DUOS):
        scores(0, s_a, duo)

    def store(chip):
        rows = pl.ds(pl.multiple_of(chip * leaf_dev, leaf_dev), leaf_dev)
        return pltpu.make_async_copy(acc.at[rows], out.at[rows], out_sem)

    def step(at, chip):
        for duo in range(DUOS):
            sums(2 * at, s_a, duo)
            scores(2 * at + 1, s_b, duo)
        for duo in range(DUOS):
            sums(2 * at + 1, s_b, duo)
            scores(2 * at + 2, s_a, duo)
        full = jnp.logical_and(chip < chips, ends[jnp.minimum(chip, chips - 1)] <= (at + 1) * 4 * DUOS)

        @pl.when(full)
        def _():
            store(chip).start()

        return jnp.where(full, chip + 1, chip)

    def flush(chip, carry):
        store(chip).start()
        return carry

    chip = lax.fori_loop(0, lax.div(count + 4 * DUOS - 1, 4 * DUOS), step, 0)
    lax.fori_loop(chip, chips, flush, 0)
    pltpu.make_async_copy(acc.at[pl.ds(0, targets)], out, out_sem).wait()


def reduce_kernel(
    part_all, out, held, send_8, recv_8, send_16, recv_16, scale_s8, scale_r8, scale_s16, scale_r16,
    load_sems, sem_s8, sem_r8, sem_s16, sem_r16,
):
    x, y, core, z = torus_position()
    leaf_dev = part_all.shape[1]
    half, part = leaf_dev // 2, leaf_dev // 4
    order = ((2, 0), (1, 1), (-1, 2), (0, 3))

    def chip_at(half_at, du, dv):
        first_x = half_at == 0
        u, v = (x, y) if first_x else (y, x)
        return pick(first_x, wrap(u + du), wrap(v + dv))

    loads = {}
    for du, _ in order:
        for dv, _ in order:
            for half_at in range(2):
                slot = chip_at(half_at, du, dv)
                ref = pl.ds(half_at * half, half)
                copy = pltpu.make_async_copy(
                    part_all.at[slot, ref], held.at[slot, ref], load_sems.at[len(loads)]
                )
                copy.start()
                loads[half_at, du, dv] = copy

    sends = []

    def wires(size, kind, chip):
        big = size == half
        pairs = (
            ((send_16, recv_16, sem_s16, sem_r16, 0), (scale_s16, scale_r16, sem_s16, sem_r16, 1))
            if big
            else ((send_8, recv_8, sem_s8, sem_r8, 0), (scale_s8, scale_r8, sem_s8, sem_r8, 1))
        )
        return [
            pltpu.make_async_remote_copy(
                src_ref=src.at[kind], dst_ref=dst.at[kind], send_sem=s.at[2 * kind + at], recv_sem=r.at[2 * kind + at],
                device_id=(chip * 2 + core, z), device_id_type=MESH,
            )
            for src, dst, s, r, at in pairs
        ]

    def unpack(size, kind, row):
        data, scale = (recv_16, scale_r16) if size == half else (recv_8, scale_r8)
        return data[kind, row].astype(jnp.int32).astype(F32) * scale[kind, pl.ds(row, 1), :]

    def send(size, kind, chip, value_at):
        data, scale = (send_16, scale_s16) if size == half else (send_8, scale_s8)

        def body(row, carry):
            value = value_at(row)
            top = jnp.maximum(jnp.max(jnp.abs(value), axis=0, keepdims=True), 1e-30)
            scale[kind, pl.ds(row, 1), :] = top * (1.0 / 32767.0)
            data[kind, row] = jnp.round(value * (32767.0 / top)).astype(jnp.int32).astype(jnp.int16)
            return carry

        lax.fori_loop(0, size, body, 0, unroll=2)
        for copy in wires(size, kind, chip):
            copy.start()
            sends.append(copy)

    def wait(size, kind):
        for copy in wires(size, kind, chip_at(0, 1, 0)):
            copy.wait_recv()

    def ready(half_at, du, dv):
        loads.pop((half_at, du, dv)).wait()

    for dv, at in order:
        for half_at in range(2):
            base = half_at * half
            ready(half_at, 2, dv)
            slot = chip_at(half_at, 2, dv)
            kind = half_at * 10 + 2 * at
            send(part, kind, chip_at(half_at, 1, 0), lambda row: held[slot, base + row])
            send(part, kind + 1, chip_at(half_at, -1, 0), lambda row: held[slot, base + part + row])
    def pass_on(dv, at):
        for half_at in range(2):
            base = half_at * half
            for du, side in ((1, 0), (-1, 1)):
                ready(half_at, du, dv)
                slot = chip_at(half_at, du, dv)
                kind = half_at * 10 + 2 * at + side
                wait(part, kind)

                def add(row, carry):
                    spot = base + side * part + row
                    held[slot, spot] = held[slot, spot] + unpack(part, kind, row)
                    return carry

                lax.fori_loop(0, part, add, 0, unroll=2)
                send(half, kind, chip_at(half_at, du, 0), lambda row: held[slot, base + row])

    def second_axis(dv, at):
        for half_at in range(2):
            base = half_at * half
            ready(half_at, 0, dv)
            slot = chip_at(half_at, 0, dv)
            kind = half_at * 10 + 2 * at
            wait(half, kind)
            wait(half, kind + 1)

            def keep(row, carry):
                held[slot, base + row] = held[slot, base + row] + unpack(half, kind, row) + unpack(half, kind + 1, row)
                return carry

            lax.fori_loop(0, half, keep, 0, unroll=2)
            if dv == 2:
                for sign, side in ((1, 0), (-1, 1)):
                    send(
                        part, half_at * 10 + 8 + side, chip_at(half_at, 0, sign),
                        lambda row: held[slot, base + side * part + row],
                    )
            elif dv != 0:
                side = 0 if dv == 1 else 1
                late = half_at * 10 + 8 + side
                wait(part, late)

                def add_late(row, carry):
                    spot = base + side * part + row
                    held[slot, spot] = held[slot, spot] + unpack(part, late, row)
                    return carry

                lax.fori_loop(0, part, add_late, 0, unroll=2)
                send(half, late, chip_at(half_at, 0, dv), lambda row: held[slot, base + row])

    for step, (dv, at) in enumerate(order):
        pass_on(dv, at)
        if step > 0:
            second_axis(*order[step - 1])
    second_axis(*order[-1])
    for half_at in range(2):
        base = half_at * half
        slot = chip_at(half_at, 0, 0)
        kind = half_at * 10 + 8
        wait(half, kind)
        wait(half, kind + 1)

        def finish(row, carry):
            out[base + row] = held[slot, base + row] + unpack(half, kind, row) + unpack(half, kind + 1, row)
            return carry

        lax.fori_loop(0, half, finish, 0, unroll=2)
    for copy in sends:
        copy.wait_send()


def per_device(points, charges, projection, skeleton_index, near_ids, far_ids):
    leaf_dev, dim, leaf = points.shape
    rhs = charges.shape[1]
    skel = skeleton_index.shape[1]
    n_z = lax.axis_size("nbr")
    chips = lax.axis_size("leaf") // 2
    cols = leaf // n_z
    near_dev, far_dev = near_ids.shape[1], far_ids.shape[1]
    sources, targets = 2 * leaf_dev, chips * leaf_dev
    params = functools.partial(pltpu.CompilerParams, vmem_limit_bytes=LIMIT)
    dma = pltpu.SemaphoreType.DMA
    shape = jax.ShapeDtypeStruct

    def row_of(ids):
        flat = ids.reshape(1, -1)
        return jnp.pad(flat, ((0, 0), (0, 128 - flat.shape[1])), constant_values=-1)

    ids = jnp.concatenate([row_of(near_ids), row_of(far_ids), jnp.full((6, 128), -1, jnp.int32)], axis=0)

    quarter = (leaf_dev // 2, rhs, 2 * skel // n_z)
    y_table, x_aug, w_skel, charges_sib, ids_all = pl.pallas_call(
        gather_kernel,
        out_shape=[
            shape((3 * sources, skel, 128), BF16),
            shape((chips, leaf_dev, 64, cols), BF16),
            shape((sources, rhs, skel), BF16),
            shape(charges.shape, BF16),
            shape((chips * n_z, 8, 128), jnp.int32),
        ],
        in_specs=[ANY] * 5,
        out_specs=[ANY] * 5,
        scratch_shapes=[
            pltpu.VMEM((2,) + points.shape, BF16),
            pltpu.VMEM((2,) + skeleton_index.shape, jnp.int32),
            pltpu.VMEM(charges.shape, BF16),
            pltpu.VMEM(projection.shape, BF16),
            pltpu.VMEM((2, n_z) + quarter, BF16),
            pltpu.VMEM((chips, leaf_dev, dim, cols), BF16),
            pltpu.VMEM((3 * sources, skel, 128), BF16),
            pltpu.VMEM((chips, leaf_dev, 64, cols), BF16),
            pltpu.VMEM((sources, rhs, skel), BF16),
            dma((40,)), dma((40,)), dma((12,)), dma((12,)), dma, dma, dma((6,)), dma((8,)),
        ],
        name="gather",
        compiler_params=params(has_side_effects=True),
    )(points, charges, projection, skeleton_index, ids)
    table = pl.pallas_call(
        functools.partial(table_kernel, leaf_dev, near_dev, far_dev, n_z),
        out_shape=shape((chips * n_z, 128), jnp.int32),
        in_specs=[VMEM],
        out_specs=VMEM,
        name="table",
        compiler_params=params(),
    )(ids_all)
    partial_sums = pl.pallas_call(
        pair_kernel,
        out_shape=shape((targets, rhs, cols), F32),
        in_specs=[SMEM] + [ANY] * 5,
        out_specs=ANY,
        scratch_shapes=[
            pltpu.VMEM((targets, 64, cols), BF16),
            pltpu.VMEM((3 * sources, skel, 128), BF16),
            pltpu.VMEM((3 * sources, rhs, skel), BF16),
            pltpu.VMEM((targets + 1, rhs, cols), F32),
            pltpu.VMEM((DUOS, skel, 2 * cols), F32),
            pltpu.VMEM((DUOS, skel, 2 * cols), F32),
            pltpu.SMEM((chips * n_z * (2 * NEAR_SLOTS + FAR_SLOTS) + 8 * DUOS,), jnp.int32),
            pltpu.SMEM((chips,), jnp.int32),
            dma((8,)),
            dma,
        ],
        name="pairs",
        compiler_params=params(),
    )(table, y_table, x_aug.reshape(targets, 64, cols), w_skel, charges, charges_sib)
    half, part = leaf_dev // 2, leaf_dev // 4
    return pl.pallas_call(
        reduce_kernel,
        out_shape=shape((leaf_dev, rhs, cols), F32),
        in_specs=[ANY],
        out_specs=VMEM,
        scratch_shapes=[
            pltpu.VMEM((chips, leaf_dev, rhs, cols), F32),
            pltpu.VMEM((20, part, rhs, cols), jnp.int16),
            pltpu.VMEM((20, part, rhs, cols), jnp.int16),
            pltpu.VMEM((20, half, rhs, cols), jnp.int16),
            pltpu.VMEM((20, half, rhs, cols), jnp.int16),
            pltpu.VMEM((20, part, cols), F32),
            pltpu.VMEM((20, part, cols), F32),
            pltpu.VMEM((20, half, cols), F32),
            pltpu.VMEM((20, half, cols), F32),
            dma((32,)), dma((40,)), dma((40,)), dma((40,)), dma((40,)),
        ],
        name="reduce",
        compiler_params=params(has_side_effects=True),
    )(partial_sums.reshape(chips, leaf_dev, rhs, cols))


def solution(mesh):
    in_specs = (
        P("leaf", None, None),
        P("leaf", None, None),
        P("leaf", "nbr", None),
        P("leaf", None),
        P("leaf", "nbr"),
        P("leaf", "nbr"),
    )
    out_specs = P("leaf", None, "nbr")
    return jax.shard_map(per_device, mesh=mesh, in_specs=in_specs, out_specs=out_specs, check_vma=False)
```

```python
import functools
import math

import jax
import jax.numpy as jnp
from jax import lax
from jax.experimental import pallas as pl
from jax.experimental.pallas import tpu as pltpu
from jax.sharding import PartitionSpec as P

MESH = pl.DeviceIdType.MESH
ANY = pl.BlockSpec(memory_space=pl.ANY)
HBM = pl.BlockSpec(memory_space=pltpu.HBM)
VMEM = pl.BlockSpec(memory_space=pltpu.VMEM)
RING = 4
NEAR_SLOTS = 6
FAR_SLOTS = 10
DUOS = 6
LIMIT = 62 * 1024 * 1000
F32 = jnp.float32
BF16 = jnp.bfloat16


def torus_position():
    leaf = lax.axis_index("leaf")
    chip = leaf // 2
    return chip // RING, chip % RING, leaf % 2, lax.axis_index("nbr")


def wrap(value):
    return lax.rem(value + 2 * RING, RING)


def pick(first_is_x, u, v):
    return u * RING + v if first_is_x else v * RING + u


def chip_table(leaf_dev, near_dev, far_dev, n_z, chip, core, ids_all):
    rows = ids_all.shape[0]
    lane = lax.broadcasted_iota(jnp.int32, (rows, 128), 1)
    row = lax.broadcasted_iota(jnp.int32, (rows, 128), 0)
    upper = lax.broadcasted_iota(jnp.int32, (128, 128), 0) <= lax.broadcasted_iota(jnp.int32, (128, 128), 1)
    upper = jnp.where(upper, 1.0, 0.0).astype(BF16)
    result = jnp.zeros((rows, 128), jnp.int32)
    for at, (per_leaf, slots, start) in enumerate(((near_dev, NEAR_SLOTS, 0), (far_dev, FAR_SLOTS, NEAR_SLOTS))):
        first = 0 if at == 0 else near_dev
        pieces = [ids_all[:, first + step, :leaf_dev] for step in range(per_leaf)]
        if per_leaf * leaf_dev < 128:
            pieces.append(jnp.full((rows, 128 - per_leaf * leaf_dev), -1, jnp.int32))
        ids = jnp.concatenate(pieces, axis=1)
        named = lax.div(ids, 2 * leaf_dev)
        member = jnp.logical_and(named == chip, ids >= 0)
        source = lax.rem(lax.rem(ids, 2 * leaf_dev) + core * leaf_dev, 2 * leaf_dev)
        code = (lax.div(row, n_z) * leaf_dev + lax.rem(lane, leaf_dev)) * 256 + source + at * 4 * leaf_dev
        flags = jnp.where(member, 1.0, 0.0)
        upto = jnp.dot(flags.astype(BF16), upper, preferred_element_type=F32).astype(jnp.int32)
        for slot in range(slots):
            chosen = jnp.logical_and(member, upto == slot + 1)
            value = jnp.sum(jnp.where(chosen, code, 0), axis=1, keepdims=True)
            result = jnp.where(lane == start + slot, value, result)
        count = jnp.sum(jnp.where(member, 1, 0), axis=1, keepdims=True)
        result = jnp.where(lane == NEAR_SLOTS + FAR_SLOTS + at, count, result)
    return result


def norm_rows(coords, sign_first):
    values = coords.astype(F32)
    norm = -jnp.sum(values * values, axis=0, keepdims=True)
    high = norm.astype(BF16).astype(F32)
    rest = norm - high
    middle = rest.astype(BF16).astype(F32)
    low = rest - middle
    shape = (16, coords.shape[1])
    row = lax.broadcasted_iota(jnp.int32, shape, 0)
    start = 0 if sign_first else 3
    ones = 3 if sign_first else 0
    result = jnp.where(jnp.logical_and(row >= ones, row < ones + 3), 1.0, 0.0)
    for at, piece in enumerate((high, middle, low)):
        result = jnp.where(row == start + at, jnp.broadcast_to(piece, shape), result)
    return result.astype(BF16)


def gather_kernel(
    near_dev, far_dev, points, charges, projection, index, ids,
    y_table, x_aug, w_table, table,
    ids_all, p_buf, i_buf, c_buf, j_buf, q_buf, x_raw,
    send_x, recv_x, send_s, recv_s, send_i, recv_i, load_sems,
):
    x, y, core, z = torus_position()
    n_z = q_buf.shape[1]
    leaf_dev, dim, leaf = points.shape
    skel = index.shape[1]
    cols = x_raw.shape[3]
    half, part = leaf_dev // 2, leaf_dev // 4
    hold = leaf_dev // 2
    piece = skel // n_z
    me = (x * RING + y) * n_z + z
    n_ids = ids_all.shape[0]
    here = x * RING + y
    own_cols = pl.ds(pl.multiple_of(z * cols, cols), cols)

    def device(chip, core_at, z_at):
        return (chip * 2 + core_at, z_at)

    barrier = pltpu.get_barrier_semaphore()

    def greet(step, carry):
        peer = lax.rem(me + step, n_ids)
        pl.semaphore_signal(
            barrier, inc=1, device_id=device(peer // n_z, core, lax.rem(peer, n_z)), device_id_type=MESH
        )
        return carry

    lax.fori_loop(1, n_ids, greet, 0)
    pl.semaphore_signal(barrier, inc=1, device_id=device(here, 1 - core, z), device_id_type=MESH)

    loads = []
    for at, (src, dst) in enumerate(
        (
            (charges, c_buf),
            (projection, j_buf),
            (points, p_buf.at[0]),
            (index, i_buf.at[0]),
            (points.at[:, :, own_cols], x_raw.at[here]),
            (ids, ids_all.at[me]),
            (charges.at[:, :, pl.ds(0, skel)], w_table.at[pl.ds(0, leaf_dev)]),
            (charges.at[:, :, pl.ds(skel, skel)], w_table.at[pl.ds(2 * leaf_dev, leaf_dev)]),
        )
    ):
        copy = pltpu.make_async_copy(src, dst, load_sems.at[at])
        copy.start()
        loads.append(copy)
    pl.semaphore_wait(barrier, n_ids)

    sends = []

    def message(kind, sems, src, dst, target):
        return pltpu.make_async_remote_copy(
            src_ref=src, dst_ref=dst, send_sem=sems[0].at[kind], recv_sem=sems[1].at[kind],
            device_id=target, device_id_type=MESH,
        )

    def start(copy):
        copy.start()
        sends.append(copy)

    side = (send_s, recv_s)
    line = (send_x, recv_x)

    own_x = []
    for half_at in range(2):
        first_x = half_at == 0
        u, v = (x, y) if first_x else (y, x)
        rows = pl.ds(half_at * half, half)
        src = points.at[rows, :, own_cols]
        dst = x_raw.at[here, rows]
        kinds = 20 * half_at
        own_x.append(
            [
                message(kinds + 0, line, src, dst, device(pick(first_x, wrap(u + 1), v), core, z)),
                message(kinds + 1, line, src, dst, device(pick(first_x, wrap(u - 1), v), core, z)),
                message(kinds + 4, line, src, dst, device(pick(first_x, u, wrap(v + 1)), core, z)),
                message(kinds + 5, line, src, dst, device(pick(first_x, u, wrap(v - 1)), core, z)),
            ]
        )
    for at in range(4):
        for half_at in range(2):
            start(own_x[half_at][at])

    sib_copies = []
    for at, (src, dst) in enumerate(
        (
            (points, p_buf.at[1]),
            (index, i_buf.at[1]),
            (charges.at[:, :, pl.ds(0, skel)], w_table.at[pl.ds(leaf_dev, leaf_dev)]),
            (charges.at[:, :, pl.ds(skel, skel)], w_table.at[pl.ds(3 * leaf_dev, leaf_dev)]),
        )
    ):
        copy = message(8 + at, side, src, dst, device(here, 1 - core, z))
        start(copy)
        sib_copies.append(copy)

    def send_ids(step, carry):
        peer = lax.rem(me + step, n_ids)
        pltpu.make_async_remote_copy(
            src_ref=ids, dst_ref=ids_all.at[me], send_sem=send_i, recv_sem=recv_i,
            device_id=device(peer // n_z, core, lax.rem(peer, n_z)), device_id_type=MESH,
        ).start()
        return carry

    lax.fori_loop(1, n_ids, send_ids, 0)

    loads[0].wait()
    loads[1].wait()

    def charge(item, carry):
        parts = []
        for at in (item, item + hold):
            parts.append(
                lax.dot_general(c_buf[at], j_buf[at], (((1,), (1,)), ((), ())), preferred_element_type=F32)
            )
        q_buf[0, z, item] = jnp.concatenate(parts, axis=1).astype(BF16)
        return carry

    lax.fori_loop(0, hold, charge, 0, unroll=2)
    z_copies = []
    own_quarter = q_buf.at[0, z]
    for step in range(1, n_z):
        copy = message(step, side, own_quarter, own_quarter, device(here, core, lax.rem(z + step, n_z)))
        start(copy)
        z_copies.append(copy)
    copy = message(0, side, own_quarter, q_buf.at[1, z], device(here, 1 - core, z))
    start(copy)
    sib_quarters = [copy]

    def item(half_at, du, dv, quarter_at=None):
        first_x = half_at == 0
        u, v = (x, y) if first_x else (y, x)
        rows = pl.ds(half_at * half, half) if quarter_at is None else pl.ds(half_at * half + quarter_at * part, part)
        return x_raw.at[pick(first_x, wrap(u + du), wrap(v + dv)), rows]

    def target(half_at, du, dv):
        first_x = half_at == 0
        u, v = (x, y) if first_x else (y, x)
        return device(pick(first_x, wrap(u + du), wrap(v + dv)), core, z)

    def arrived(half_at, kind, ref):
        message(20 * half_at + kind, line, ref, ref, target(half_at, 1, 0)).wait_recv()

    def forward(half_at, kind, ref, du, dv):
        start(message(20 * half_at + kind, line, ref, ref, target(half_at, du, dv)))

    def across(half_at, slot, du):
        ref = item(half_at, du, 0)
        forward(half_at, 4 + 4 * slot, ref, 0, 1)
        forward(half_at, 5 + 4 * slot, ref, 0, -1)

    def relay(half_at, slot, du):
        arrived(half_at, 4 + 4 * slot, item(half_at, du, -1))
        forward(half_at, 6 + 4 * slot, item(half_at, du, -1, 0), 0, 1)
        arrived(half_at, 5 + 4 * slot, item(half_at, du, 1))
        forward(half_at, 7 + 4 * slot, item(half_at, du, 1, 1), 0, -1)

    pad = jnp.zeros((16, cols), BF16)

    def widen(half_at, du, dv):
        first_x = half_at == 0
        u, v = (x, y) if first_x else (y, x)
        chip = pick(first_x, wrap(u + du), wrap(v + dv))
        base = half_at * half

        def body(at, carry):
            coords = x_raw[chip, base + at]
            x_aug[chip, base + at] = jnp.concatenate([coords, norm_rows(coords, True), pad], axis=0)
            return carry

        lax.fori_loop(0, half, body, 0, unroll=4)

    wide_pad = jnp.zeros((16, leaf), BF16)
    point_number = lax.broadcasted_iota(jnp.int32, (leaf, skel), 0)
    sources = 2 * leaf_dev

    def source(at_side, first, count):
        def body(at, carry):
            coords = p_buf[at_side, at]
            block = jnp.concatenate([coords + coords, norm_rows(coords, False), wide_pad], axis=0)
            block = jnp.concatenate([block, block], axis=0)
            turned = block.T
            row = at_side * leaf_dev + at
            y_table[row] = turned[:skel]
            y_table[sources + row] = turned[skel:]
            chosen = point_number == i_buf[at_side, pl.ds(at, 1), :]
            chosen = jnp.where(chosen, 1.0, 0.0).astype(BF16)
            picked = jnp.dot(block, chosen, preferred_element_type=F32).astype(BF16)
            y_table[2 * sources + row] = picked.T
            return carry

        lax.fori_loop(first, first + count, body, 0, unroll=2)

    def assemble(at_side):
        def body(at, carry):
            chunks = [q_buf[at_side, step, at] for step in range(n_z)]
            for half_at in range(2):
                pieces = [chunk[:, half_at * piece : (half_at + 1) * piece] for chunk in chunks]
                w_table[2 * sources + at_side * leaf_dev + half_at * hold + at] = jnp.concatenate(pieces, axis=1)
            return carry

        lax.fori_loop(0, hold, body, 0, unroll=2)

    for half_at in range(2):
        arrived(half_at, 0, item(half_at, -1, 0))
        forward(half_at, 2, item(half_at, -1, 0, 0), 1, 0)
        across(half_at, 1, -1)
    for half_at in range(2):
        arrived(half_at, 1, item(half_at, 1, 0))
        forward(half_at, 3, item(half_at, 1, 0, 1), -1, 0)
        across(half_at, 2, 1)
    for half_at in range(2):
        relay(half_at, 0, 0)
    loads[2].wait()
    loads[3].wait()
    loads[4].wait()
    source(0, 0, leaf_dev // 2)
    for half_at in range(2):
        arrived(half_at, 2, item(half_at, 2, 0, 0))
        arrived(half_at, 3, item(half_at, 2, 0, 1))
        across(half_at, 3, 2)
    for step in range(1, n_z):
        z_copies[step - 1].wait_recv()
        slot = lax.rem(z - step + n_z, n_z)
        copy = message(4 + step, side, q_buf.at[0, slot], q_buf.at[1, slot], device(here, 1 - core, z))
        start(copy)
        sib_quarters.append(copy)
    source(0, leaf_dev // 2, leaf_dev // 2)
    for half_at in range(2):
        relay(half_at, 1, -1)
    sib_copies[0].wait_recv()
    sib_copies[1].wait_recv()
    source(1, 0, leaf_dev // 2)
    for half_at in range(2):
        relay(half_at, 2, 1)
    source(1, leaf_dev // 2, leaf_dev // 2)
    for copy in loads[5:]:
        copy.wait()
    sib_copies[2].wait_recv()
    sib_copies[3].wait_recv()
    others = ids_all.at[pl.ds(0, n_ids - 1)]
    every = pltpu.make_async_remote_copy(
        src_ref=others, dst_ref=others, send_sem=send_i, recv_sem=recv_i,
        device_id=target(0, 1, 0), device_id_type=MESH,
    )
    every.wait_send()
    every.wait_recv()
    table[...] = chip_table(leaf_dev, near_dev, far_dev, n_z, here, core, ids_all)
    for half_at in range(2):
        for du in (0, -1, 1, 2):
            widen(half_at, du, 0)
    for half_at in range(2):
        relay(half_at, 3, 2)
    assemble(0)
    for copy in sib_quarters:
        copy.wait_recv()
    assemble(1)
    for half_at in range(2):
        for dv in (-1, 1):
            for du in (0, -1, 1, 2):
                widen(half_at, du, dv)
    for slot, du in ((0, 0), (1, -1), (2, 1), (3, 2)):
        for half_at in range(2):
            arrived(half_at, 6 + 4 * slot, item(half_at, du, 2, 0))
            arrived(half_at, 7 + 4 * slot, item(half_at, du, 2, 1))
            widen(half_at, du, 2)
    for copy in sends:
        copy.wait_send()


def pair_kernel(table_in, y_table, x_aug, w_table, out, acc, s_a, s_b, table, items, ends, out_sem):
    copy = pltpu.make_async_copy(table_in, table, out_sem)
    copy.start()
    skel = y_table.shape[1]
    targets, _, cols = x_aug.shape
    leaf_dev = w_table.shape[0] // 6
    n_z = table.shape[0] // (targets // leaf_dev)
    sources = 2 * leaf_dev

    def zero(at, carry):
        acc[at] = jnp.zeros(acc.shape[1:], F32)
        return carry

    lax.fori_loop(0, targets + 1, zero, 0, unroll=4)
    copy.wait()

    def fill(chip, count):
        for step in range(n_z):
            row = chip * n_z + step
            for slot in range(NEAR_SLOTS):
                code = table[row, slot]
                items[count + 2 * slot] = code
                items[count + 2 * slot + 1] = code + sources
            count = count + 2 * table[row, NEAR_SLOTS + FAR_SLOTS]
            for slot in range(FAR_SLOTS):
                items[count + slot] = table[row, NEAR_SLOTS + slot]
            count = count + table[row, NEAR_SLOTS + FAR_SLOTS + 1]
        ends[chip] = count
        return count

    chips = table.shape[0] // n_z
    count = lax.fori_loop(0, chips, fill, 0)
    for at in range(6 * DUOS):
        items[count + at] = targets * 256


    empty = jnp.zeros((64, cols), BF16)
    low_lanes = lax.broadcasted_iota(jnp.int32, (skel, 128), 1) < 64

    def read(at):
        code = items[at]
        return lax.shift_right_logical(code, 8), jnp.bitwise_and(code, 255)

    def scores(group, buf, at):
        for duo in [at]:
            t_0, u_0 = read(group * 2 * DUOS + 2 * duo)
            t_1, u_1 = read(group * 2 * DUOS + 2 * duo + 1)
            x_0 = x_aug[jnp.minimum(t_0, targets - 1)]
            x_1 = x_aug[jnp.minimum(t_1, targets - 1)]
            right = jnp.concatenate(
                [jnp.concatenate([x_0, empty], axis=0), jnp.concatenate([empty, x_1], axis=0)], axis=1
            )
            left = jnp.where(low_lanes, y_table[u_0], y_table[u_1])
            buf[duo] = jnp.dot(left, right, preferred_element_type=F32)

    def sums(group, buf, at):
        for duo in [at]:
            t_0, u_0 = read(group * 2 * DUOS + 2 * duo)
            t_1, u_1 = read(group * 2 * DUOS + 2 * duo + 1)
            kernel = jnp.exp(buf[duo]).astype(BF16)
            weights = jnp.concatenate([w_table[u_0], w_table[u_1]], axis=0)
            terms = jnp.dot(weights, kernel, preferred_element_type=F32)
            rhs = terms.shape[0] // 2
            acc[t_0] = acc[t_0] + terms[:rhs, :cols]
            acc[t_1] = acc[t_1] + terms[rhs:, cols:]

    for duo in range(DUOS):
        scores(0, s_a, duo)

    def store(chip):
        rows = pl.ds(pl.multiple_of(chip * leaf_dev, leaf_dev), leaf_dev)
        return pltpu.make_async_copy(acc.at[rows], out.at[rows], out_sem)

    def step(at, chip):
        for duo in range(DUOS):
            sums(2 * at, s_a, duo)
            scores(2 * at + 1, s_b, duo)
        for duo in range(DUOS):
            sums(2 * at + 1, s_b, duo)
            scores(2 * at + 2, s_a, duo)
        full = jnp.logical_and(chip < chips, ends[jnp.minimum(chip, chips - 1)] <= (at + 1) * 4 * DUOS)

        @pl.when(full)
        def _():
            store(chip).start()

        return jnp.where(full, chip + 1, chip)

    def flush(chip, carry):
        store(chip).start()
        return carry

    chip = lax.fori_loop(0, lax.div(count + 4 * DUOS - 1, 4 * DUOS), step, 0)
    lax.fori_loop(chip, chips, flush, 0)
    pltpu.make_async_copy(acc.at[pl.ds(0, targets)], out, out_sem).wait()


def reduce_kernel(
    part_all, out, held, send_8, recv_8, send_16, recv_16, scale_s8, scale_r8, scale_s16, scale_r16,
    load_sems, sem_s8, sem_r8, sem_s16, sem_r16,
):
    x, y, core, z = torus_position()
    leaf_dev = part_all.shape[1]
    half, part = leaf_dev // 2, leaf_dev // 4
    order = ((2, 0), (1, 1), (-1, 2), (0, 3))

    def chip_at(half_at, du, dv):
        first_x = half_at == 0
        u, v = (x, y) if first_x else (y, x)
        return pick(first_x, wrap(u + du), wrap(v + dv))

    barrier = pltpu.get_barrier_semaphore()
    for du, dv in ((1, 0), (-1, 0), (0, 1), (0, -1)):
        pl.semaphore_signal(
            barrier, inc=1, device_id=(chip_at(0, du, dv) * 2 + core, z), device_id_type=MESH
        )

    loads = {}
    for du, _ in order:
        for dv, _ in order:
            for half_at in range(2):
                slot = chip_at(half_at, du, dv)
                ref = pl.ds(half_at * half, half)
                copy = pltpu.make_async_copy(
                    part_all.at[slot, ref], held.at[slot, ref], load_sems.at[len(loads)]
                )
                copy.start()
                loads[half_at, du, dv] = copy

    pl.semaphore_wait(barrier, 4)
    sends = []

    def wires(size, kind, chip):
        big = size == half
        pairs = (
            ((send_16, recv_16, sem_s16, sem_r16, 0), (scale_s16, scale_r16, sem_s16, sem_r16, 1))
            if big
            else ((send_8, recv_8, sem_s8, sem_r8, 0), (scale_s8, scale_r8, sem_s8, sem_r8, 1))
        )
        return [
            pltpu.make_async_remote_copy(
                src_ref=src.at[kind], dst_ref=dst.at[kind], send_sem=s.at[2 * kind + at], recv_sem=r.at[2 * kind + at],
                device_id=(chip * 2 + core, z), device_id_type=MESH,
            )
            for src, dst, s, r, at in pairs
        ]

    def unpack(size, kind, row):
        data, scale = (recv_16, scale_r16) if size == half else (recv_8, scale_r8)
        return data[kind, row].astype(jnp.int32).astype(F32) * scale[kind, pl.ds(row, 1), :]

    def send(size, kind, chip, value_at):
        data, scale = (send_16, scale_s16) if size == half else (send_8, scale_s8)

        def body(row, carry):
            value = value_at(row)
            top = jnp.maximum(jnp.max(jnp.abs(value), axis=0, keepdims=True), 1e-30)
            scale[kind, pl.ds(row, 1), :] = top * (1.0 / 32767.0)
            data[kind, row] = jnp.round(value * (32767.0 / top)).astype(jnp.int32).astype(jnp.int16)
            return carry

        lax.fori_loop(0, size, body, 0, unroll=2)
        for copy in wires(size, kind, chip):
            copy.start()
            sends.append(copy)

    def wait(size, kind):
        for copy in wires(size, kind, chip_at(0, 1, 0)):
            copy.wait_recv()

    def ready(half_at, du, dv):
        loads.pop((half_at, du, dv)).wait()

    for dv, at in order:
        for half_at in range(2):
            base = half_at * half
            ready(half_at, 2, dv)
            slot = chip_at(half_at, 2, dv)
            kind = half_at * 10 + 2 * at
            send(part, kind, chip_at(half_at, 1, 0), lambda row: held[slot, base + row])
            send(part, kind + 1, chip_at(half_at, -1, 0), lambda row: held[slot, base + part + row])
    def pass_on(dv, at):
        for half_at in range(2):
            base = half_at * half
            for du, side in ((1, 0), (-1, 1)):
                ready(half_at, du, dv)
                slot = chip_at(half_at, du, dv)
                kind = half_at * 10 + 2 * at + side
                wait(part, kind)

                def add(row, carry):
                    spot = base + side * part + row
                    held[slot, spot] = held[slot, spot] + unpack(part, kind, row)
                    return carry

                lax.fori_loop(0, part, add, 0, unroll=2)
                send(half, kind, chip_at(half_at, du, 0), lambda row: held[slot, base + row])

    def second_axis(dv, at):
        for half_at in range(2):
            base = half_at * half
            ready(half_at, 0, dv)
            slot = chip_at(half_at, 0, dv)
            kind = half_at * 10 + 2 * at
            wait(half, kind)
            wait(half, kind + 1)

            def keep(row, carry):
                held[slot, base + row] = held[slot, base + row] + unpack(half, kind, row) + unpack(half, kind + 1, row)
                return carry

            lax.fori_loop(0, half, keep, 0, unroll=2)
            if dv == 2:
                for sign, side in ((1, 0), (-1, 1)):
                    send(
                        part, half_at * 10 + 8 + side, chip_at(half_at, 0, sign),
                        lambda row: held[slot, base + side * part + row],
                    )
            elif dv != 0:
                side = 0 if dv == 1 else 1
                late = half_at * 10 + 8 + side
                wait(part, late)

                def add_late(row, carry):
                    spot = base + side * part + row
                    held[slot, spot] = held[slot, spot] + unpack(part, late, row)
                    return carry

                lax.fori_loop(0, part, add_late, 0, unroll=2)
                send(half, late, chip_at(half_at, 0, dv), lambda row: held[slot, base + row])

    for step, (dv, at) in enumerate(order):
        pass_on(dv, at)
        if step > 0:
            second_axis(*order[step - 1])
    second_axis(*order[-1])
    for half_at in range(2):
        base = half_at * half
        slot = chip_at(half_at, 0, 0)
        kind = half_at * 10 + 8
        wait(half, kind)
        wait(half, kind + 1)

        def finish(row, carry):
            out[base + row] = held[slot, base + row] + unpack(half, kind, row) + unpack(half, kind + 1, row)
            return carry

        lax.fori_loop(0, half, finish, 0, unroll=2)
    for copy in sends:
        copy.wait_send()


def per_device(points, charges, projection, skeleton_index, near_ids, far_ids):
    leaf_dev, dim, leaf = points.shape
    rhs = charges.shape[1]
    skel = skeleton_index.shape[1]
    n_z = lax.axis_size("nbr")
    chips = lax.axis_size("leaf") // 2
    cols = leaf // n_z
    near_dev, far_dev = near_ids.shape[1], far_ids.shape[1]
    sources, targets = 2 * leaf_dev, chips * leaf_dev
    params = pltpu.CompilerParams
    dma = pltpu.SemaphoreType.DMA
    shape = jax.ShapeDtypeStruct

    ids = jnp.concatenate([near_ids.T, far_ids.T], axis=0)
    ids = jnp.pad(ids, ((0, 8 - near_dev - far_dev), (0, 128 - leaf_dev)), constant_values=-1)

    quarter = (leaf_dev // 2, rhs, 2 * skel // n_z)
    y_table, x_aug, w_table, table = pl.pallas_call(
        functools.partial(gather_kernel, near_dev, far_dev),
        out_shape=[
            pltpu.VMEM((3 * sources, skel, 128), BF16),
            pltpu.VMEM((chips, leaf_dev, 64, cols), BF16),
            pltpu.VMEM((3 * sources, rhs, skel), BF16),
            pltpu.VMEM((chips * n_z, 128), jnp.int32),
        ],
        in_specs=[HBM] * 5,
        out_specs=[VMEM] * 4,
        scratch_shapes=[
            pltpu.VMEM((chips * n_z, 8, 128), jnp.int32),
            pltpu.VMEM((2,) + points.shape, BF16),
            pltpu.VMEM((2,) + skeleton_index.shape, jnp.int32),
            pltpu.VMEM(charges.shape, BF16),
            pltpu.VMEM(projection.shape, BF16),
            pltpu.VMEM((2, n_z) + quarter, BF16),
            pltpu.VMEM((chips, leaf_dev, dim, cols), BF16),
            dma((40,)), dma((40,)), dma((12,)), dma((12,)), dma, dma, dma((8,)),
        ],
        name="gather",
        compiler_params=params(has_side_effects=True, collective_id=0, vmem_limit_bytes=28 << 20),
    )(*[pltpu.with_memory_space_constraint(value, pltpu.HBM) for value in (points, charges, projection, skeleton_index, ids)])
    tables = [table, y_table, x_aug.reshape(targets, 64, cols), w_table]
    partial_sums = pl.pallas_call(
        pair_kernel,
        out_shape=shape((targets, rhs, cols), F32),
        in_specs=[VMEM] * 4,
        out_specs=ANY,
        scratch_shapes=[
            pltpu.VMEM((targets + 1, rhs, cols), F32),
            pltpu.VMEM((DUOS, skel, 2 * cols), F32),
            pltpu.VMEM((DUOS, skel, 2 * cols), F32),
            pltpu.SMEM((chips * n_z, 128), jnp.int32),
            pltpu.SMEM((chips * n_z * (2 * NEAR_SLOTS + FAR_SLOTS) + 8 * DUOS,), jnp.int32),
            pltpu.SMEM((chips,), jnp.int32),
            dma,
        ],
        name="pairs",
        compiler_params=params(vmem_limit_bytes=28 << 20),
    )(*[pltpu.with_memory_space_constraint(value, pltpu.VMEM) for value in tables])
    half, part = leaf_dev // 2, leaf_dev // 4
    return pl.pallas_call(
        reduce_kernel,
        out_shape=shape((leaf_dev, rhs, cols), F32),
        in_specs=[ANY],
        out_specs=VMEM,
        scratch_shapes=[
            pltpu.VMEM((chips, leaf_dev, rhs, cols), F32),
            pltpu.VMEM((20, part, rhs, cols), jnp.int16),
            pltpu.VMEM((20, part, rhs, cols), jnp.int16),
            pltpu.VMEM((20, half, rhs, cols), jnp.int16),
            pltpu.VMEM((20, half, rhs, cols), jnp.int16),
            pltpu.VMEM((20, part, cols), F32),
            pltpu.VMEM((20, part, cols), F32),
            pltpu.VMEM((20, half, cols), F32),
            pltpu.VMEM((20, half, cols), F32),
            dma((32,)), dma((40,)), dma((40,)), dma((40,)), dma((40,)),
        ],
        name="reduce",
        compiler_params=params(has_side_effects=True, collective_id=1, vmem_limit_bytes=LIMIT),
    )(partial_sums.reshape(chips, leaf_dev, rhs, cols))


def solution(mesh):
    in_specs = (
        P("leaf", None, None),
        P("leaf", None, None),
        P("leaf", "nbr", None),
        P("leaf", None),
        P("leaf", "nbr"),
        P("leaf", "nbr"),
    )
    out_specs = P("leaf", None, "nbr")
    return jax.shard_map(per_device, mesh=mesh, in_specs=in_specs, out_specs=out_specs, check_vma=False)
```

```python
import functools
import math

import jax
import jax.numpy as jnp
from jax import lax
from jax.experimental import pallas as pl
from jax.experimental.pallas import tpu as pltpu
from jax.sharding import PartitionSpec as P

MESH = pl.DeviceIdType.MESH
HBM = pl.BlockSpec(memory_space=pltpu.HBM)
VMEM = pl.BlockSpec(memory_space=pltpu.VMEM)
RING = 4
NEAR_SLOTS = 6
FAR_SLOTS = 10
DUOS = 6
F32 = jnp.float32
BF16 = jnp.bfloat16


def torus_position():
    leaf = lax.axis_index("leaf")
    chip = leaf // 2
    return chip // RING, chip % RING, leaf % 2, lax.axis_index("nbr")


def wrap(value):
    return lax.rem(value + 2 * RING, RING)


def pick(first_is_x, u, v):
    return u * RING + v if first_is_x else v * RING + u


def chip_table(leaf_dev, near_dev, far_dev, n_z, chip, core, ids_all):
    rows = ids_all.shape[0]
    lane = lax.broadcasted_iota(jnp.int32, (rows, 128), 1)
    row = lax.broadcasted_iota(jnp.int32, (rows, 128), 0)
    upper = lax.broadcasted_iota(jnp.int32, (128, 128), 0) <= lax.broadcasted_iota(jnp.int32, (128, 128), 1)
    upper = jnp.where(upper, 1.0, 0.0).astype(BF16)
    result = jnp.zeros((rows, 128), jnp.int32)
    for at, (per_leaf, slots, start) in enumerate(((near_dev, NEAR_SLOTS, 0), (far_dev, FAR_SLOTS, NEAR_SLOTS))):
        first = 0 if at == 0 else near_dev
        pieces = [ids_all[:, first + step, :leaf_dev] for step in range(per_leaf)]
        if per_leaf * leaf_dev < 128:
            pieces.append(jnp.full((rows, 128 - per_leaf * leaf_dev), -1, jnp.int32))
        ids = jnp.concatenate(pieces, axis=1)
        named = lax.div(ids, 2 * leaf_dev)
        member = jnp.logical_and(named == chip, ids >= 0)
        source = lax.rem(lax.rem(ids, 2 * leaf_dev) + core * leaf_dev, 2 * leaf_dev)
        code = (lax.div(row, n_z) * leaf_dev + lax.rem(lane, leaf_dev)) * 256 + source + at * 4 * leaf_dev
        flags = jnp.where(member, 1.0, 0.0)
        upto = jnp.dot(flags.astype(BF16), upper, preferred_element_type=F32).astype(jnp.int32)
        for slot in range(slots):
            chosen = jnp.logical_and(member, upto == slot + 1)
            value = jnp.sum(jnp.where(chosen, code, 0), axis=1, keepdims=True)
            result = jnp.where(lane == start + slot, value, result)
        count = jnp.sum(jnp.where(member, 1, 0), axis=1, keepdims=True)
        result = jnp.where(lane == NEAR_SLOTS + FAR_SLOTS + at, count, result)
    return result


def norm_rows(coords, sign_first):
    values = coords.astype(F32)
    norm = -jnp.sum(values * values, axis=0, keepdims=True)
    high = norm.astype(BF16).astype(F32)
    rest = norm - high
    middle = rest.astype(BF16).astype(F32)
    low = rest - middle
    shape = (16, coords.shape[1])
    row = lax.broadcasted_iota(jnp.int32, shape, 0)
    start = 0 if sign_first else 3
    ones = 3 if sign_first else 0
    result = jnp.where(jnp.logical_and(row >= ones, row < ones + 3), 1.0, 0.0)
    for at, piece in enumerate((high, middle, low)):
        result = jnp.where(row == start + at, jnp.broadcast_to(piece, shape), result)
    return result.astype(BF16)


def gather_kernel(
    points, charges, projection, index, near_t, far_t,
    y_table, x_aug, w_table, table,
    ids, ids_all, p_buf, i_buf, c_buf, j_buf, q_buf, x_raw,
    send_x, recv_x, send_s, recv_s, send_i, recv_i, load_sems,
):
    x, y, core, z = torus_position()
    n_z = q_buf.shape[1]
    near_dev, far_dev = near_t.shape[0], far_t.shape[0]
    leaf_dev, dim, leaf = points.shape
    skel = index.shape[1]
    cols = x_raw.shape[3]
    half, part = leaf_dev // 2, leaf_dev // 4
    hold = leaf_dev // 2
    piece = skel // n_z
    me = (x * RING + y) * n_z + z
    n_ids = ids_all.shape[0]
    here = x * RING + y
    own_cols = pl.ds(pl.multiple_of(z * cols, cols), cols)

    def device(chip, core_at, z_at):
        return (chip * 2 + core_at, z_at)

    barrier = pltpu.get_barrier_semaphore()

    def greet(step, carry):
        peer = lax.rem(me + step, n_ids)
        pl.semaphore_signal(
            barrier, inc=1, device_id=device(peer // n_z, core, lax.rem(peer, n_z)), device_id_type=MESH
        )
        return carry

    lax.fori_loop(1, n_ids, greet, 0)
    pl.semaphore_signal(barrier, inc=1, device_id=device(here, 1 - core, z), device_id_type=MESH)

    loads = []
    for at, (src, dst) in enumerate(
        (
            (charges, c_buf),
            (projection, j_buf),
            (points, p_buf.at[0]),
            (index, i_buf.at[0]),
            (points.at[:, :, own_cols], x_raw.at[here]),
            (charges.at[:, :, pl.ds(0, skel)], w_table.at[pl.ds(0, leaf_dev)]),
            (charges.at[:, :, pl.ds(skel, skel)], w_table.at[pl.ds(2 * leaf_dev, leaf_dev)]),
        )
    ):
        copy = pltpu.make_async_copy(src, dst, load_sems.at[at])
        copy.start()
        loads.append(copy)

    blank = jnp.full(ids.shape, -1, jnp.int32)
    ids[...] = blank
    ids[:near_dev, :leaf_dev] = near_t[...]
    ids[near_dev : near_dev + far_dev, :leaf_dev] = far_t[...]

    loads[0].wait()
    loads[1].wait()

    def charge(item, carry):
        parts = []
        for at in (item, item + hold):
            parts.append(
                lax.dot_general(c_buf[at], j_buf[at], (((1,), (1,)), ((), ())), preferred_element_type=F32)
            )
        q_buf[0, z, item] = jnp.concatenate(parts, axis=1).astype(BF16)
        return carry

    lax.fori_loop(0, hold, charge, 0, unroll=2)
    pl.semaphore_wait(barrier, n_ids)
    sends = []

    def message(kind, sems, src, dst, target):
        return pltpu.make_async_remote_copy(
            src_ref=src, dst_ref=dst, send_sem=sems[0].at[kind], recv_sem=sems[1].at[kind],
            device_id=target, device_id_type=MESH,
        )

    def start(copy):
        copy.start()
        sends.append(copy)

    side = (send_s, recv_s)
    line = (send_x, recv_x)

    own_x = []
    for half_at in range(2):
        first_x = half_at == 0
        u, v = (x, y) if first_x else (y, x)
        rows = pl.ds(half_at * half, half)
        src = points.at[rows, :, own_cols]
        dst = x_raw.at[here, rows]
        kinds = 20 * half_at
        own_x.append(
            [
                message(kinds + 0, line, src, dst, device(pick(first_x, wrap(u + 1), v), core, z)),
                message(kinds + 1, line, src, dst, device(pick(first_x, wrap(u - 1), v), core, z)),
                message(kinds + 4, line, src, dst, device(pick(first_x, u, wrap(v + 1)), core, z)),
                message(kinds + 5, line, src, dst, device(pick(first_x, u, wrap(v - 1)), core, z)),
            ]
        )
    for at in range(4):
        for half_at in range(2):
            start(own_x[half_at][at])

    sib_copies = []
    for at, (src, dst) in enumerate(
        (
            (points, p_buf.at[1]),
            (index, i_buf.at[1]),
            (charges.at[:, :, pl.ds(0, skel)], w_table.at[pl.ds(leaf_dev, leaf_dev)]),
            (charges.at[:, :, pl.ds(skel, skel)], w_table.at[pl.ds(3 * leaf_dev, leaf_dev)]),
        )
    ):
        copy = message(8 + at, side, src, dst, device(here, 1 - core, z))
        start(copy)
        sib_copies.append(copy)

    def send_ids(step, carry):
        peer = lax.rem(me + step, n_ids)
        pltpu.make_async_remote_copy(
            src_ref=ids, dst_ref=ids_all.at[me], send_sem=send_i, recv_sem=recv_i,
            device_id=device(peer // n_z, core, lax.rem(peer, n_z)), device_id_type=MESH,
        ).start()
        return carry

    lax.fori_loop(1, n_ids, send_ids, 0)

    z_copies = []
    own_quarter = q_buf.at[0, z]
    for step in range(1, n_z):
        copy = message(step, side, own_quarter, own_quarter, device(here, core, lax.rem(z + step, n_z)))
        start(copy)
        z_copies.append(copy)
    copy = message(0, side, own_quarter, q_buf.at[1, z], device(here, 1 - core, z))
    start(copy)
    sib_quarters = [copy]

    def item(half_at, du, dv, quarter_at=None):
        first_x = half_at == 0
        u, v = (x, y) if first_x else (y, x)
        rows = pl.ds(half_at * half, half) if quarter_at is None else pl.ds(half_at * half + quarter_at * part, part)
        return x_raw.at[pick(first_x, wrap(u + du), wrap(v + dv)), rows]

    def target(half_at, du, dv):
        first_x = half_at == 0
        u, v = (x, y) if first_x else (y, x)
        return device(pick(first_x, wrap(u + du), wrap(v + dv)), core, z)

    def arrived(half_at, kind, ref):
        message(20 * half_at + kind, line, ref, ref, target(half_at, 1, 0)).wait_recv()

    def forward(half_at, kind, ref, du, dv):
        start(message(20 * half_at + kind, line, ref, ref, target(half_at, du, dv)))

    def across(half_at, slot, du):
        ref = item(half_at, du, 0)
        forward(half_at, 4 + 4 * slot, ref, 0, 1)
        forward(half_at, 5 + 4 * slot, ref, 0, -1)

    def relay(half_at, slot, du):
        arrived(half_at, 4 + 4 * slot, item(half_at, du, -1))
        forward(half_at, 6 + 4 * slot, item(half_at, du, -1, 0), 0, 1)
        arrived(half_at, 5 + 4 * slot, item(half_at, du, 1))
        forward(half_at, 7 + 4 * slot, item(half_at, du, 1, 1), 0, -1)

    pad = jnp.zeros((16, cols), BF16)

    def widen(half_at, du, dv):
        first_x = half_at == 0
        u, v = (x, y) if first_x else (y, x)
        chip = pick(first_x, wrap(u + du), wrap(v + dv))
        base = half_at * half

        def body(at, carry):
            coords = x_raw[chip, base + at]
            x_aug[chip, base + at] = jnp.concatenate([coords, norm_rows(coords, True), pad], axis=0)
            return carry

        lax.fori_loop(0, half, body, 0, unroll=4)

    wide_pad = jnp.zeros((16, leaf), BF16)
    point_number = lax.broadcasted_iota(jnp.int32, (leaf, skel), 0)
    sources = 2 * leaf_dev

    def source(at_side, first, count):
        def body(at, carry):
            coords = p_buf[at_side, at]
            block = jnp.concatenate([coords + coords, norm_rows(coords, False), wide_pad], axis=0)
            block = jnp.concatenate([block, block], axis=0)
            turned = block.T
            row = at_side * leaf_dev + at
            y_table[row] = turned[:skel]
            y_table[sources + row] = turned[skel:]
            chosen = point_number == i_buf[at_side, pl.ds(at, 1), :]
            chosen = jnp.where(chosen, 1.0, 0.0).astype(BF16)
            picked = jnp.dot(block, chosen, preferred_element_type=F32).astype(BF16)
            y_table[2 * sources + row] = picked.T
            return carry

        lax.fori_loop(first, first + count, body, 0, unroll=2)

    def assemble(at_side):
        def body(at, carry):
            chunks = [q_buf[at_side, step, at] for step in range(n_z)]
            for half_at in range(2):
                pieces = [chunk[:, half_at * piece : (half_at + 1) * piece] for chunk in chunks]
                w_table[2 * sources + at_side * leaf_dev + half_at * hold + at] = jnp.concatenate(pieces, axis=1)
            return carry

        lax.fori_loop(0, hold, body, 0, unroll=2)

    for half_at in range(2):
        arrived(half_at, 0, item(half_at, -1, 0))
        forward(half_at, 2, item(half_at, -1, 0, 0), 1, 0)
        across(half_at, 1, -1)
    for half_at in range(2):
        arrived(half_at, 1, item(half_at, 1, 0))
        forward(half_at, 3, item(half_at, 1, 0, 1), -1, 0)
        across(half_at, 2, 1)
    for half_at in range(2):
        relay(half_at, 0, 0)
    loads[2].wait()
    loads[3].wait()
    loads[4].wait()
    source(0, 0, leaf_dev // 2)
    for half_at in range(2):
        arrived(half_at, 2, item(half_at, 2, 0, 0))
        arrived(half_at, 3, item(half_at, 2, 0, 1))
        across(half_at, 3, 2)
    for step in range(1, n_z):
        z_copies[step - 1].wait_recv()
        slot = lax.rem(z - step + n_z, n_z)
        copy = message(4 + step, side, q_buf.at[0, slot], q_buf.at[1, slot], device(here, 1 - core, z))
        start(copy)
        sib_quarters.append(copy)
    source(0, leaf_dev // 2, leaf_dev // 2)
    for half_at in range(2):
        relay(half_at, 1, -1)
    sib_copies[0].wait_recv()
    sib_copies[1].wait_recv()
    source(1, 0, leaf_dev // 2)
    for half_at in range(2):
        relay(half_at, 2, 1)
    source(1, leaf_dev // 2, leaf_dev // 2)
    for copy in loads[5:]:
        copy.wait()
    sib_copies[2].wait_recv()
    sib_copies[3].wait_recv()
    ids_all[me] = ids[...]
    others = ids_all.at[pl.ds(0, n_ids - 1)]
    every = pltpu.make_async_remote_copy(
        src_ref=others, dst_ref=others, send_sem=send_i, recv_sem=recv_i,
        device_id=target(0, 1, 0), device_id_type=MESH,
    )
    every.wait_send()
    every.wait_recv()
    table[...] = chip_table(leaf_dev, near_dev, far_dev, n_z, here, core, ids_all)
    for half_at in range(2):
        for du in (0, -1, 1, 2):
            widen(half_at, du, 0)
    for half_at in range(2):
        relay(half_at, 3, 2)
    assemble(0)
    for copy in sib_quarters:
        copy.wait_recv()
    assemble(1)
    for half_at in range(2):
        for dv in (-1, 1):
            for du in (0, -1, 1, 2):
                widen(half_at, du, dv)
    for slot, du in ((0, 0), (1, -1), (2, 1), (3, 2)):
        for half_at in range(2):
            arrived(half_at, 6 + 4 * slot, item(half_at, du, 2, 0))
            arrived(half_at, 7 + 4 * slot, item(half_at, du, 2, 1))
            widen(half_at, du, 2)
    for copy in sends:
        copy.wait_send()


def pair_kernel(table_in, y_table, x_aug, w_table, acc, s_a, s_b, table, items, load_sem):
    copy = pltpu.make_async_copy(table_in, table, load_sem)
    copy.start()
    skel = y_table.shape[1]
    targets, _, cols = x_aug.shape
    leaf_dev = w_table.shape[0] // 6
    n_z = table.shape[0] // (targets // leaf_dev)
    sources = 2 * leaf_dev

    def zero(at, carry):
        acc[at] = jnp.zeros(acc.shape[1:], F32)
        return carry

    lax.fori_loop(0, targets + 1, zero, 0, unroll=4)
    copy.wait()

    def fill(chip, count):
        for step in range(n_z):
            row = chip * n_z + step
            for slot in range(NEAR_SLOTS):
                code = table[row, slot]
                items[count + 2 * slot] = code
                items[count + 2 * slot + 1] = code + sources
            count = count + 2 * table[row, NEAR_SLOTS + FAR_SLOTS]
            for slot in range(FAR_SLOTS):
                items[count + slot] = table[row, NEAR_SLOTS + slot]
            count = count + table[row, NEAR_SLOTS + FAR_SLOTS + 1]
        return count

    chips = table.shape[0] // n_z
    count = lax.fori_loop(0, chips, fill, 0)
    for at in range(6 * DUOS):
        items[count + at] = targets * 256


    empty = jnp.zeros((64, cols), BF16)
    low_lanes = lax.broadcasted_iota(jnp.int32, (skel, 128), 1) < 64

    def read(at):
        code = items[at]
        return lax.shift_right_logical(code, 8), jnp.bitwise_and(code, 255)

    def scores(group, buf, at):
        for duo in [at]:
            t_0, u_0 = read(group * 2 * DUOS + 2 * duo)
            t_1, u_1 = read(group * 2 * DUOS + 2 * duo + 1)
            x_0 = x_aug[jnp.minimum(t_0, targets - 1)]
            x_1 = x_aug[jnp.minimum(t_1, targets - 1)]
            right = jnp.concatenate(
                [jnp.concatenate([x_0, empty], axis=0), jnp.concatenate([empty, x_1], axis=0)], axis=1
            )
            left = jnp.where(low_lanes, y_table[u_0], y_table[u_1])
            buf[duo] = jnp.dot(left, right, preferred_element_type=F32)

    def sums(group, buf, at):
        for duo in [at]:
            t_0, u_0 = read(group * 2 * DUOS + 2 * duo)
            t_1, u_1 = read(group * 2 * DUOS + 2 * duo + 1)
            kernel = jnp.exp(buf[duo]).astype(BF16)
            weights = jnp.concatenate([w_table[u_0], w_table[u_1]], axis=0)
            terms = jnp.dot(weights, kernel, preferred_element_type=F32)
            rhs = terms.shape[0] // 2
            acc[t_0] = acc[t_0] + terms[:rhs, :cols]
            acc[t_1] = acc[t_1] + terms[rhs:, cols:]

    for duo in range(DUOS):
        scores(0, s_a, duo)

    def step(at, carry):
        for duo in range(DUOS):
            sums(2 * at, s_a, duo)
            scores(2 * at + 1, s_b, duo)
        for duo in range(DUOS):
            sums(2 * at + 1, s_b, duo)
            scores(2 * at + 2, s_a, duo)
        return carry

    lax.fori_loop(0, lax.div(count + 4 * DUOS - 1, 4 * DUOS), step, 0)


def reduce_kernel(
    leaf_dev, held, out, send_8, recv_8, send_16, recv_16, scale_s8, scale_r8, scale_s16, scale_r16,
    sem_s8, sem_r8, sem_s16, sem_r16,
):
    x, y, core, z = torus_position()
    half, part = leaf_dev // 2, leaf_dev // 4
    order = ((2, 0), (1, 1), (-1, 2), (0, 3))

    def chip_at(half_at, du, dv):
        first_x = half_at == 0
        u, v = (x, y) if first_x else (y, x)
        return pick(first_x, wrap(u + du), wrap(v + dv))

    barrier = pltpu.get_barrier_semaphore()
    for du, dv in ((1, 0), (-1, 0), (0, 1), (0, -1)):
        pl.semaphore_signal(
            barrier, inc=1, device_id=(chip_at(0, du, dv) * 2 + core, z), device_id_type=MESH
        )

    pl.semaphore_wait(barrier, 4)
    sends = []

    def wires(size, kind, chip):
        big = size == half
        pairs = (
            ((send_16, recv_16, sem_s16, sem_r16, 0), (scale_s16, scale_r16, sem_s16, sem_r16, 1))
            if big
            else ((send_8, recv_8, sem_s8, sem_r8, 0), (scale_s8, scale_r8, sem_s8, sem_r8, 1))
        )
        return [
            pltpu.make_async_remote_copy(
                src_ref=src.at[kind], dst_ref=dst.at[kind], send_sem=s.at[2 * kind + at], recv_sem=r.at[2 * kind + at],
                device_id=(chip * 2 + core, z), device_id_type=MESH,
            )
            for src, dst, s, r, at in pairs
        ]

    def unpack(size, kind, row):
        data, scale = (recv_16, scale_r16) if size == half else (recv_8, scale_r8)
        return data[kind, row].astype(jnp.int32).astype(F32) * scale[kind, pl.ds(row, 1), :]

    def code(size, kind, first, count, value_at):
        data, scale = (send_16, scale_s16) if size == half else (send_8, scale_s8)

        def body(row, carry):
            value = value_at(row)
            top = jnp.maximum(jnp.max(jnp.abs(value), axis=0, keepdims=True), 1e-30)
            scale[kind, pl.ds(row, 1), :] = top * (1.0 / 32767.0)
            data[kind, row] = jnp.round(value * (32767.0 / top)).astype(jnp.int32).astype(jnp.int16)
            return carry

        lax.fori_loop(first, first + count, body, 0, unroll=2)

    def send(size, kind, chip):
        for copy in wires(size, kind, chip):
            copy.start()
            sends.append(copy)

    def wait(size, kind):
        for copy in wires(size, kind, chip_at(0, 1, 0)):
            copy.wait_recv()

    def local(half_at, du, dv):
        start = chip_at(half_at, du, dv) * leaf_dev + half_at * half
        return lambda row: held[start + row]

    for dv, at in order:
        for half_at in range(2):
            kind = half_at * 10 + 2 * at
            mine = local(half_at, 2, dv)
            for side, du in ((0, 1), (1, -1)):
                code(part, kind + side, 0, part, lambda row: mine(side * part + row))
                send(part, kind + side, chip_at(half_at, du, 0))

    def add_part(kind, side, mine):
        wait(part, kind)
        low = side * part
        code(half, kind, low, part, lambda row: mine(row) + unpack(part, kind, row - low))

    def pass_on(dv, at):
        for half_at in range(2):
            for du, side in ((1, 0), (-1, 1)):
                kind = half_at * 10 + 2 * at + side
                mine = local(half_at, du, dv)
                code(half, kind, part - side * part, part, mine)
                add_part(kind, side, mine)
                send(half, kind, chip_at(half_at, du, 0))

    def column(half_at, dv, at):
        kind = half_at * 10 + 2 * at
        mine = local(half_at, 0, dv)
        wait(half, kind)
        wait(half, kind + 1)
        return lambda row: mine(row) + unpack(half, kind, row) + unpack(half, kind + 1, row)

    def second_axis(dv, at):
        for half_at in range(2):
            total = column(half_at, dv, at)
            if dv == 2:
                for sign, side in ((1, 0), (-1, 1)):
                    late = half_at * 10 + 8 + side
                    code(part, late, 0, part, lambda row: total(side * part + row))
                    send(part, late, chip_at(half_at, 0, sign))
            else:
                side = 0 if dv == 1 else 1
                late = half_at * 10 + 8 + side
                code(half, late, part - side * part, part, total)
                add_part(late, side, total)
                send(half, late, chip_at(half_at, 0, dv))

    for step, (dv, at) in enumerate(order):
        pass_on(dv, at)
        if step > 0:
            second_axis(*order[step - 1])
    for half_at in range(2):
        base = half_at * half
        total = column(half_at, *order[-1])
        kind = half_at * 10 + 8
        wait(half, kind)
        wait(half, kind + 1)

        def finish(row, carry):
            out[base + row] = total(row) + unpack(half, kind, row) + unpack(half, kind + 1, row)
            return carry

        lax.fori_loop(0, half, finish, 0, unroll=2)
    for copy in sends:
        copy.wait_send()


def per_device(points, charges, projection, skeleton_index, near_ids, far_ids):
    leaf_dev, dim, leaf = points.shape
    rhs = charges.shape[1]
    skel = skeleton_index.shape[1]
    n_z = lax.axis_size("nbr")
    chips = lax.axis_size("leaf") // 2
    cols = leaf // n_z
    near_dev, far_dev = near_ids.shape[1], far_ids.shape[1]
    sources, targets = 2 * leaf_dev, chips * leaf_dev
    params = pltpu.CompilerParams
    dma = pltpu.SemaphoreType.DMA
    shape = jax.ShapeDtypeStruct

    quarter = (leaf_dev // 2, rhs, 2 * skel // n_z)
    y_table, x_aug, w_table, table = pl.pallas_call(
        gather_kernel,
        out_shape=[
            pltpu.VMEM((3 * sources, skel, 128), BF16),
            pltpu.VMEM((chips, leaf_dev, 64, cols), BF16),
            pltpu.VMEM((3 * sources, rhs, skel), BF16),
            pltpu.VMEM((chips * n_z, 128), jnp.int32),
        ],
        in_specs=[HBM] * 4 + [VMEM] * 2,
        out_specs=[VMEM] * 4,
        scratch_shapes=[
            pltpu.VMEM((8, 128), jnp.int32),
            pltpu.VMEM((chips * n_z, 8, 128), jnp.int32),
            pltpu.VMEM((2,) + points.shape, BF16),
            pltpu.VMEM((2,) + skeleton_index.shape, jnp.int32),
            pltpu.VMEM(charges.shape, BF16),
            pltpu.VMEM(projection.shape, BF16),
            pltpu.VMEM((2, n_z) + quarter, BF16),
            pltpu.VMEM((chips, leaf_dev, dim, cols), BF16),
            dma((40,)), dma((40,)), dma((12,)), dma((12,)), dma, dma, dma((8,)),
        ],
        name="gather",
        compiler_params=params(has_side_effects=True, collective_id=0, vmem_limit_bytes=17 << 20),
    )(
        *[
            pltpu.with_memory_space_constraint(value, pltpu.HBM)
            for value in (points, charges, projection, skeleton_index)
        ],
        near_ids.T,
        far_ids.T,
    )
    tables = [table, y_table, x_aug.reshape(targets, 64, cols), w_table]
    partial_sums = pl.pallas_call(
        pair_kernel,
        out_shape=pltpu.VMEM((targets + 1, rhs, cols), F32),
        in_specs=[VMEM] * 4,
        out_specs=VMEM,
        scratch_shapes=[
            pltpu.VMEM((DUOS, skel, 2 * cols), F32),
            pltpu.VMEM((DUOS, skel, 2 * cols), F32),
            pltpu.SMEM((chips * n_z, 128), jnp.int32),
            pltpu.SMEM((chips * n_z * (2 * NEAR_SLOTS + FAR_SLOTS) + 8 * DUOS,), jnp.int32),
            dma,
        ],
        name="pairs",
        compiler_params=params(vmem_limit_bytes=6 << 20),
    )(*[pltpu.with_memory_space_constraint(value, pltpu.VMEM) for value in tables])
    half, part = leaf_dev // 2, leaf_dev // 4
    return pl.pallas_call(
        functools.partial(reduce_kernel, leaf_dev),
        out_shape=pltpu.VMEM((leaf_dev, rhs, cols), F32),
        in_specs=[VMEM],
        out_specs=VMEM,
        scratch_shapes=[
            pltpu.VMEM((20, part, rhs, cols), jnp.int16),
            pltpu.VMEM((20, part, rhs, cols), jnp.int16),
            pltpu.VMEM((20, half, rhs, cols), jnp.int16),
            pltpu.VMEM((20, half, rhs, cols), jnp.int16),
            pltpu.VMEM((20, part, cols), F32),
            pltpu.VMEM((20, part, cols), F32),
            pltpu.VMEM((20, half, cols), F32),
            pltpu.VMEM((20, half, cols), F32),
            dma((40,)), dma((40,)), dma((40,)), dma((40,)),
        ],
        name="reduce",
        compiler_params=params(has_side_effects=True, collective_id=1, vmem_limit_bytes=17 << 20),
    )(pltpu.with_memory_space_constraint(partial_sums, pltpu.VMEM))


def solution(mesh):
    in_specs = (
        P("leaf", None, None),
        P("leaf", None, None),
        P("leaf", "nbr", None),
        P("leaf", None),
        P("leaf", "nbr"),
        P("leaf", "nbr"),
    )
    out_specs = P("leaf", None, "nbr")
    return jax.shard_map(per_device, mesh=mesh, in_specs=in_specs, out_specs=out_specs, check_vma=False)
```

```python
import functools
import math

import jax
import jax.numpy as jnp
from jax import lax
from jax.experimental import pallas as pl
from jax.experimental.pallas import tpu as pltpu
from jax.sharding import PartitionSpec as P

MESH = pl.DeviceIdType.MESH
HBM = pl.BlockSpec(memory_space=pltpu.HBM)
VMEM = pl.BlockSpec(memory_space=pltpu.VMEM)
RING = 4
NEAR_SLOTS = 6
FAR_SLOTS = 10
DUOS = 6
F32 = jnp.float32
BF16 = jnp.bfloat16


def torus_position():
    leaf = lax.axis_index("leaf")
    chip = leaf // 2
    return chip // RING, chip % RING, leaf % 2, lax.axis_index("nbr")


def wrap(value):
    return lax.rem(value + 2 * RING, RING)


def pick(first_is_x, u, v):
    return u * RING + v if first_is_x else v * RING + u


def chip_table(leaf_dev, near_dev, far_dev, n_z, chip, core, ids_all):
    rows = ids_all.shape[0]
    lane = lax.broadcasted_iota(jnp.int32, (rows, 128), 1)
    row = lax.broadcasted_iota(jnp.int32, (rows, 128), 0)
    upper = lax.broadcasted_iota(jnp.int32, (128, 128), 0) <= lax.broadcasted_iota(jnp.int32, (128, 128), 1)
    upper = jnp.where(upper, 1.0, 0.0).astype(BF16)
    result = jnp.zeros((rows, 128), jnp.int32)
    for at, (per_leaf, slots, start) in enumerate(((near_dev, NEAR_SLOTS, 0), (far_dev, FAR_SLOTS, NEAR_SLOTS))):
        first = 0 if at == 0 else near_dev
        pieces = [ids_all[:, first + step, :leaf_dev] for step in range(per_leaf)]
        if per_leaf * leaf_dev < 128:
            pieces.append(jnp.full((rows, 128 - per_leaf * leaf_dev), -1, jnp.int32))
        ids = jnp.concatenate(pieces, axis=1)
        named = lax.div(ids, 2 * leaf_dev)
        member = jnp.logical_and(named == chip, ids >= 0)
        source = lax.rem(lax.rem(ids, 2 * leaf_dev) + core * leaf_dev, 2 * leaf_dev)
        code = (lax.div(row, n_z) * leaf_dev + lax.rem(lane, leaf_dev)) * 256 + source + at * 4 * leaf_dev
        flags = jnp.where(member, 1.0, 0.0)
        upto = jnp.dot(flags.astype(BF16), upper, preferred_element_type=F32).astype(jnp.int32)
        for slot in range(slots):
            chosen = jnp.logical_and(member, upto == slot + 1)
            value = jnp.sum(jnp.where(chosen, code, 0), axis=1, keepdims=True)
            result = jnp.where(lane == start + slot, value, result)
        count = jnp.sum(jnp.where(member, 1, 0), axis=1, keepdims=True)
        result = jnp.where(lane == NEAR_SLOTS + FAR_SLOTS + at, count, result)
    return result


def norm_rows(coords, sign_first):
    values = coords.astype(F32)
    norm = -jnp.sum(values * values, axis=0, keepdims=True)
    high = norm.astype(BF16).astype(F32)
    rest = norm - high
    middle = rest.astype(BF16).astype(F32)
    low = rest - middle
    shape = (16, coords.shape[1])
    row = lax.broadcasted_iota(jnp.int32, shape, 0)
    start = 0 if sign_first else 3
    ones = 3 if sign_first else 0
    result = jnp.where(jnp.logical_and(row >= ones, row < ones + 3), 1.0, 0.0)
    for at, piece in enumerate((high, middle, low)):
        result = jnp.where(row == start + at, jnp.broadcast_to(piece, shape), result)
    return result.astype(BF16)


def gather_kernel(
    points, charges, projection, index, near_in, far_in,
    y_table, x_aug, w_table, table,
    near_t, far_t, ids, ids_all, p_buf, i_buf, c_buf, j_buf, q_buf, x_raw,
    send_x, recv_x, send_s, recv_s, send_i, recv_i, load_sems,
):
    x, y, core, z = torus_position()
    n_z = q_buf.shape[1]
    near_dev, far_dev = near_t.shape[0], far_t.shape[0]
    leaf_dev, dim, leaf = points.shape
    skel = index.shape[1]
    cols = x_raw.shape[3]
    half, part = leaf_dev // 2, leaf_dev // 4
    hold = leaf_dev // 2
    piece = skel // n_z
    me = (x * RING + y) * n_z + z
    n_ids = ids_all.shape[0]
    here = x * RING + y
    own_cols = pl.ds(pl.multiple_of(z * cols, cols), cols)

    def device(chip, core_at, z_at):
        return (chip * 2 + core_at, z_at)

    barrier = pltpu.get_barrier_semaphore()

    peers = []
    for dx in range(RING):
        for dy in range(RING):
            chip = wrap(x + dx) * RING + wrap(y + dy)
            for dz in range(n_z):
                if dx or dy or dz:
                    peers.append(device(chip, core, lax.rem(z + dz, n_z)))
    for peer in peers:
        pl.semaphore_signal(barrier, inc=1, device_id=peer, device_id_type=MESH)
    pl.semaphore_signal(barrier, inc=1, device_id=device(here, 1 - core, z), device_id_type=MESH)

    loads = []
    for at, (src, dst) in enumerate(
        (
            (charges, c_buf),
            (projection, j_buf),
            (points, p_buf.at[0]),
            (index, i_buf.at[0]),
            (points.at[:, :, own_cols], x_raw.at[here]),
            (charges.at[:, :, pl.ds(0, skel)], w_table.at[pl.ds(0, leaf_dev)]),
            (charges.at[:, :, pl.ds(skel, skel)], w_table.at[pl.ds(2 * leaf_dev, leaf_dev)]),
            (near_in, near_t),
            (far_in, far_t),
        )
    ):
        copy = pltpu.make_async_copy(src, dst, load_sems.at[at])
        copy.start()
        loads.append(copy)

    blank = jnp.full(ids.shape, -1, jnp.int32)
    ids[...] = blank
    loads[7].wait()
    loads[8].wait()
    ids[:near_dev, :leaf_dev] = near_t[...]
    ids[near_dev : near_dev + far_dev, :leaf_dev] = far_t[...]

    loads[0].wait()
    loads[1].wait()

    def charge(item, carry):
        parts = []
        for at in (item, item + hold):
            parts.append(
                lax.dot_general(c_buf[at], j_buf[at], (((1,), (1,)), ((), ())), preferred_element_type=F32)
            )
        q_buf[0, z, item] = jnp.concatenate(parts, axis=1).astype(BF16)
        return carry

    lax.fori_loop(0, hold, charge, 0, unroll=2)
    pl.semaphore_wait(barrier, n_ids)
    sends = []

    def message(kind, sems, src, dst, target):
        return pltpu.make_async_remote_copy(
            src_ref=src, dst_ref=dst, send_sem=sems[0].at[kind], recv_sem=sems[1].at[kind],
            device_id=target, device_id_type=MESH,
        )

    def start(copy):
        copy.start()
        sends.append(copy)

    side = (send_s, recv_s)
    line = (send_x, recv_x)

    own_x = []
    for half_at in range(2):
        first_x = half_at == 0
        u, v = (x, y) if first_x else (y, x)
        rows = pl.ds(half_at * half, half)
        src = points.at[rows, :, own_cols]
        dst = x_raw.at[here, rows]
        kinds = 20 * half_at
        own_x.append(
            [
                message(kinds + 0, line, src, dst, device(pick(first_x, wrap(u + 1), v), core, z)),
                message(kinds + 1, line, src, dst, device(pick(first_x, wrap(u - 1), v), core, z)),
                message(kinds + 4, line, src, dst, device(pick(first_x, u, wrap(v + 1)), core, z)),
                message(kinds + 5, line, src, dst, device(pick(first_x, u, wrap(v - 1)), core, z)),
            ]
        )
    for at in range(4):
        for half_at in range(2):
            start(own_x[half_at][at])

    sib_copies = []
    for at, (src, dst) in enumerate(
        (
            (points, p_buf.at[1]),
            (index, i_buf.at[1]),
            (charges.at[:, :, pl.ds(0, skel)], w_table.at[pl.ds(leaf_dev, leaf_dev)]),
            (charges.at[:, :, pl.ds(skel, skel)], w_table.at[pl.ds(3 * leaf_dev, leaf_dev)]),
        )
    ):
        copy = message(8 + at, side, src, dst, device(here, 1 - core, z))
        start(copy)
        sib_copies.append(copy)

    z_copies = []
    own_quarter = q_buf.at[0, z]
    for step in range(1, n_z):
        copy = message(step, side, own_quarter, own_quarter, device(here, core, lax.rem(z + step, n_z)))
        start(copy)
        z_copies.append(copy)
    copy = message(0, side, own_quarter, q_buf.at[1, z], device(here, 1 - core, z))
    start(copy)
    sib_quarters = [copy]

    for peer in peers:
        pltpu.make_async_remote_copy(
            src_ref=ids, dst_ref=ids_all.at[me], send_sem=send_i, recv_sem=recv_i,
            device_id=peer, device_id_type=MESH,
        ).start()

    def item(half_at, du, dv, quarter_at=None):
        first_x = half_at == 0
        u, v = (x, y) if first_x else (y, x)
        rows = pl.ds(half_at * half, half) if quarter_at is None else pl.ds(half_at * half + quarter_at * part, part)
        return x_raw.at[pick(first_x, wrap(u + du), wrap(v + dv)), rows]

    def target(half_at, du, dv):
        first_x = half_at == 0
        u, v = (x, y) if first_x else (y, x)
        return device(pick(first_x, wrap(u + du), wrap(v + dv)), core, z)

    def arrived(half_at, kind, ref):
        message(20 * half_at + kind, line, ref, ref, target(half_at, 1, 0)).wait_recv()

    def forward(half_at, kind, ref, du, dv):
        start(message(20 * half_at + kind, line, ref, ref, target(half_at, du, dv)))

    def across(half_at, slot, du):
        ref = item(half_at, du, 0)
        forward(half_at, 4 + 4 * slot, ref, 0, 1)
        forward(half_at, 5 + 4 * slot, ref, 0, -1)

    def relay(half_at, slot, du):
        arrived(half_at, 4 + 4 * slot, item(half_at, du, -1))
        forward(half_at, 6 + 4 * slot, item(half_at, du, -1, 0), 0, 1)
        arrived(half_at, 5 + 4 * slot, item(half_at, du, 1))
        forward(half_at, 7 + 4 * slot, item(half_at, du, 1, 1), 0, -1)

    pad = jnp.zeros((16, cols), BF16)

    def widen(half_at, du, dv):
        first_x = half_at == 0
        u, v = (x, y) if first_x else (y, x)
        chip = pick(first_x, wrap(u + du), wrap(v + dv))
        base = half_at * half

        def body(at, carry):
            coords = x_raw[chip, base + at]
            x_aug[chip, base + at] = jnp.concatenate([coords, norm_rows(coords, True), pad], axis=0)
            return carry

        lax.fori_loop(0, half, body, 0, unroll=4)

    wide_pad = jnp.zeros((16, leaf), BF16)
    point_number = lax.broadcasted_iota(jnp.int32, (leaf, skel), 0)
    sources = 2 * leaf_dev

    def source(at_side, first, count):
        def body(at, carry):
            coords = p_buf[at_side, at]
            block = jnp.concatenate([coords + coords, norm_rows(coords, False), wide_pad], axis=0)
            block = jnp.concatenate([block, block], axis=0)
            turned = block.T
            row = at_side * leaf_dev + at
            y_table[row] = turned[:skel]
            y_table[sources + row] = turned[skel:]
            chosen = point_number == i_buf[at_side, pl.ds(at, 1), :]
            chosen = jnp.where(chosen, 1.0, 0.0).astype(BF16)
            picked = jnp.dot(block, chosen, preferred_element_type=F32).astype(BF16)
            y_table[2 * sources + row] = picked.T
            return carry

        lax.fori_loop(first, first + count, body, 0, unroll=4)

    def assemble(at_side):
        def body(at, carry):
            chunks = [q_buf[at_side, step, at] for step in range(n_z)]
            for half_at in range(2):
                pieces = [chunk[:, half_at * piece : (half_at + 1) * piece] for chunk in chunks]
                w_table[2 * sources + at_side * leaf_dev + half_at * hold + at] = jnp.concatenate(pieces, axis=1)
            return carry

        lax.fori_loop(0, hold, body, 0, unroll=2)

    for copy in loads[2:5]:
        copy.wait()
    source(0, 0, leaf_dev // 2)
    for half_at in range(2):
        arrived(half_at, 0, item(half_at, -1, 0))
        forward(half_at, 2, item(half_at, -1, 0, 0), 1, 0)
        across(half_at, 1, -1)
    for half_at in range(2):
        arrived(half_at, 1, item(half_at, 1, 0))
        forward(half_at, 3, item(half_at, 1, 0, 1), -1, 0)
        across(half_at, 2, 1)
    source(0, leaf_dev // 2, leaf_dev // 2)
    for half_at in range(2):
        relay(half_at, 0, 0)
    for step in range(1, n_z):
        z_copies[step - 1].wait_recv()
        slot = lax.rem(z - step + n_z, n_z)
        copy = message(4 + step, side, q_buf.at[0, slot], q_buf.at[1, slot], device(here, 1 - core, z))
        start(copy)
        sib_quarters.append(copy)
    sib_copies[0].wait_recv()
    sib_copies[1].wait_recv()
    source(1, 0, leaf_dev // 2)
    for half_at in range(2):
        arrived(half_at, 2, item(half_at, 2, 0, 0))
        arrived(half_at, 3, item(half_at, 2, 0, 1))
        across(half_at, 3, 2)
    source(1, leaf_dev // 2, leaf_dev // 2)
    for half_at in range(2):
        relay(half_at, 1, -1)
    for half_at in range(2):
        for du in (0, -1, 1, 2):
            widen(half_at, du, 0)
    for half_at in range(2):
        relay(half_at, 2, 1)
    for copy in loads[5:7]:
        copy.wait()
    sib_copies[2].wait_recv()
    sib_copies[3].wait_recv()
    assemble(0)
    for copy in sib_quarters:
        copy.wait_recv()
    assemble(1)
    for half_at in range(2):
        relay(half_at, 3, 2)
    ids_all[me] = ids[...]
    others = ids_all.at[pl.ds(0, n_ids - 1)]
    every = pltpu.make_async_remote_copy(
        src_ref=others, dst_ref=others, send_sem=send_i, recv_sem=recv_i,
        device_id=target(0, 1, 0), device_id_type=MESH,
    )
    every.wait_send()
    every.wait_recv()
    table[...] = chip_table(leaf_dev, near_dev, far_dev, n_z, here, core, ids_all)
    for half_at in range(2):
        for dv in (-1, 1):
            for du in (0, -1, 1, 2):
                widen(half_at, du, dv)
    for slot, du in ((0, 0), (1, -1), (2, 1), (3, 2)):
        for half_at in range(2):
            arrived(half_at, 6 + 4 * slot, item(half_at, du, 2, 0))
            arrived(half_at, 7 + 4 * slot, item(half_at, du, 2, 1))
            widen(half_at, du, 2)
    for copy in sends:
        copy.wait_send()


def pair_kernel(table_in, y_table, x_aug, w_table, acc, s_a, s_b, table, items, load_sem):
    copy = pltpu.make_async_copy(table_in, table, load_sem)
    copy.start()
    skel = y_table.shape[1]
    targets, _, cols = x_aug.shape
    leaf_dev = w_table.shape[0] // 6
    n_z = table.shape[0] // (targets // leaf_dev)
    sources = 2 * leaf_dev

    def zero(at, carry):
        acc[at] = jnp.zeros(acc.shape[1:], F32)
        return carry

    lax.fori_loop(0, targets + 1, zero, 0, unroll=4)
    copy.wait()

    def fill(chip, count):
        for step in range(n_z):
            row = chip * n_z + step
            for slot in range(NEAR_SLOTS):
                code = table[row, slot]
                items[count + 2 * slot] = code
                items[count + 2 * slot + 1] = code + sources
            count = count + 2 * table[row, NEAR_SLOTS + FAR_SLOTS]
            for slot in range(FAR_SLOTS):
                items[count + slot] = table[row, NEAR_SLOTS + slot]
            count = count + table[row, NEAR_SLOTS + FAR_SLOTS + 1]
        return count

    chips = table.shape[0] // n_z
    count = lax.fori_loop(0, chips, fill, 0)
    for at in range(6 * DUOS):
        items[count + at] = targets * 256


    empty = jnp.zeros((64, cols), BF16)
    low_lanes = lax.broadcasted_iota(jnp.int32, (skel, 128), 1) < 64

    def read(at):
        code = items[at]
        return lax.shift_right_logical(code, 8), jnp.bitwise_and(code, 255)

    def scores(group, buf, at):
        for duo in [at]:
            t_0, u_0 = read(group * 2 * DUOS + 2 * duo)
            t_1, u_1 = read(group * 2 * DUOS + 2 * duo + 1)
            x_0 = x_aug[jnp.minimum(t_0, targets - 1)]
            x_1 = x_aug[jnp.minimum(t_1, targets - 1)]
            right = jnp.concatenate(
                [jnp.concatenate([x_0, empty], axis=0), jnp.concatenate([empty, x_1], axis=0)], axis=1
            )
            left = jnp.where(low_lanes, y_table[u_0], y_table[u_1])
            buf[duo] = jnp.dot(left, right, preferred_element_type=F32)

    def sums(group, buf, at):
        for duo in [at]:
            t_0, u_0 = read(group * 2 * DUOS + 2 * duo)
            t_1, u_1 = read(group * 2 * DUOS + 2 * duo + 1)
            kernel = jnp.exp(buf[duo]).astype(BF16)
            weights = jnp.concatenate([w_table[u_0], w_table[u_1]], axis=0)
            terms = jnp.dot(weights, kernel, preferred_element_type=F32)
            rhs = terms.shape[0] // 2
            acc[t_0] = acc[t_0] + terms[:rhs, :cols]
            acc[t_1] = acc[t_1] + terms[rhs:, cols:]

    for duo in range(DUOS):
        scores(0, s_a, duo)

    def step(at, carry):
        for duo in range(DUOS):
            sums(2 * at, s_a, duo)
            scores(2 * at + 1, s_b, duo)
        for duo in range(DUOS):
            sums(2 * at + 1, s_b, duo)
            scores(2 * at + 2, s_a, duo)
        return carry

    lax.fori_loop(0, lax.div(count + 4 * DUOS - 1, 4 * DUOS), step, 0)


def reduce_kernel(
    leaf_dev, held, out, send_8, recv_8, send_16, recv_16, scale_s8, scale_r8, scale_s16, scale_r16,
    sem_s8, sem_r8, sem_s16, sem_r16,
):
    x, y, core, z = torus_position()
    half, part = leaf_dev // 2, leaf_dev // 4
    order = ((2, 0), (1, 1), (-1, 2), (0, 3))

    def chip_at(half_at, du, dv):
        first_x = half_at == 0
        u, v = (x, y) if first_x else (y, x)
        return pick(first_x, wrap(u + du), wrap(v + dv))

    barrier = pltpu.get_barrier_semaphore()
    for du, dv in ((1, 0), (-1, 0), (0, 1), (0, -1)):
        pl.semaphore_signal(
            barrier, inc=1, device_id=(chip_at(0, du, dv) * 2 + core, z), device_id_type=MESH
        )

    pl.semaphore_wait(barrier, 4)
    sends = []

    def wires(size, kind, chip):
        big = size == half
        pairs = (
            ((send_16, recv_16, sem_s16, sem_r16, 0), (scale_s16, scale_r16, sem_s16, sem_r16, 1))
            if big
            else ((send_8, recv_8, sem_s8, sem_r8, 0), (scale_s8, scale_r8, sem_s8, sem_r8, 1))
        )
        return [
            pltpu.make_async_remote_copy(
                src_ref=src.at[kind], dst_ref=dst.at[kind], send_sem=s.at[2 * kind + at], recv_sem=r.at[2 * kind + at],
                device_id=(chip * 2 + core, z), device_id_type=MESH,
            )
            for src, dst, s, r, at in pairs
        ]

    def unpack(size, kind, row):
        data, scale = (recv_16, scale_r16) if size == half else (recv_8, scale_r8)
        return data[kind, row].astype(jnp.int32).astype(F32) * scale[kind, pl.ds(row, 1), :]

    def code(size, kind, first, count, value_at):
        data, scale = (send_16, scale_s16) if size == half else (send_8, scale_s8)

        def body(row, carry):
            value = value_at(row)
            top = jnp.maximum(jnp.max(jnp.abs(value), axis=0, keepdims=True), 1e-30)
            scale[kind, pl.ds(row, 1), :] = top * (1.0 / 32767.0)
            data[kind, row] = jnp.round(value * (32767.0 / top)).astype(jnp.int32).astype(jnp.int16)
            return carry

        lax.fori_loop(first, first + count, body, 0, unroll=2)

    def send(size, kind, chip):
        for copy in wires(size, kind, chip):
            copy.start()
            sends.append(copy)

    def wait(size, kind):
        for copy in wires(size, kind, chip_at(0, 1, 0)):
            copy.wait_recv()

    def local(half_at, du, dv):
        start = chip_at(half_at, du, dv) * leaf_dev + half_at * half
        return lambda row: held[start + row]

    for dv, at in order:
        for half_at in range(2):
            kind = half_at * 10 + 2 * at
            mine = local(half_at, 2, dv)
            for side, du in ((0, 1), (1, -1)):
                code(part, kind + side, 0, part, lambda row: mine(side * part + row))
                send(part, kind + side, chip_at(half_at, du, 0))

    def add_part(kind, side, mine):
        wait(part, kind)
        low = side * part
        code(half, kind, low, part, lambda row: mine(row) + unpack(part, kind, row - low))

    def pass_on(dv, at):
        for half_at in range(2):
            for du, side in ((1, 0), (-1, 1)):
                kind = half_at * 10 + 2 * at + side
                mine = local(half_at, du, dv)
                code(half, kind, part - side * part, part, mine)
                add_part(kind, side, mine)
                send(half, kind, chip_at(half_at, du, 0))

    def column(half_at, dv, at):
        kind = half_at * 10 + 2 * at
        mine = local(half_at, 0, dv)
        wait(half, kind)
        wait(half, kind + 1)
        return lambda row: mine(row) + unpack(half, kind, row) + unpack(half, kind + 1, row)

    def second_axis(dv, at):
        for half_at in range(2):
            total = column(half_at, dv, at)
            if dv == 2:
                for sign, side in ((1, 0), (-1, 1)):
                    late = half_at * 10 + 8 + side
                    code(part, late, 0, part, lambda row: total(side * part + row))
                    send(part, late, chip_at(half_at, 0, sign))
            else:
                side = 0 if dv == 1 else 1
                late = half_at * 10 + 8 + side
                code(half, late, part - side * part, part, total)
                add_part(late, side, total)
                send(half, late, chip_at(half_at, 0, dv))

    for step, (dv, at) in enumerate(order):
        pass_on(dv, at)
        if step > 0:
            second_axis(*order[step - 1])
    for half_at in range(2):
        base = half_at * half
        total = column(half_at, *order[-1])
        kind = half_at * 10 + 8
        wait(half, kind)
        wait(half, kind + 1)

        def finish(row, carry):
            out[base + row] = total(row) + unpack(half, kind, row) + unpack(half, kind + 1, row)
            return carry

        lax.fori_loop(0, half, finish, 0, unroll=2)
    for copy in sends:
        copy.wait_send()


def per_device(points, charges, projection, skeleton_index, near_ids, far_ids):
    leaf_dev, dim, leaf = points.shape
    rhs = charges.shape[1]
    skel = skeleton_index.shape[1]
    n_z = lax.axis_size("nbr")
    chips = lax.axis_size("leaf") // 2
    cols = leaf // n_z
    near_dev, far_dev = near_ids.shape[1], far_ids.shape[1]
    sources, targets = 2 * leaf_dev, chips * leaf_dev
    params = pltpu.CompilerParams
    dma = pltpu.SemaphoreType.DMA
    shape = jax.ShapeDtypeStruct

    quarter = (leaf_dev // 2, rhs, 2 * skel // n_z)
    y_table, x_aug, w_table, table = pl.pallas_call(
        gather_kernel,
        out_shape=[
            pltpu.VMEM((3 * sources, skel, 128), BF16),
            pltpu.VMEM((chips, leaf_dev, 64, cols), BF16),
            pltpu.VMEM((3 * sources, rhs, skel), BF16),
            pltpu.VMEM((chips * n_z, 128), jnp.int32),
        ],
        in_specs=[HBM] * 6,
        out_specs=[VMEM] * 4,
        scratch_shapes=[
            pltpu.VMEM((near_dev, leaf_dev), jnp.int32),
            pltpu.VMEM((far_dev, leaf_dev), jnp.int32),
            pltpu.VMEM((8, 128), jnp.int32),
            pltpu.VMEM((chips * n_z, 8, 128), jnp.int32),
            pltpu.VMEM((2,) + points.shape, BF16),
            pltpu.VMEM((2,) + skeleton_index.shape, jnp.int32),
            pltpu.VMEM(charges.shape, BF16),
            pltpu.VMEM(projection.shape, BF16),
            pltpu.VMEM((2, n_z) + quarter, BF16),
            pltpu.VMEM((chips, leaf_dev, dim, cols), BF16),
            dma((40,)), dma((40,)), dma((12,)), dma((12,)), dma, dma, dma((9,)),
        ],
        name="gather",
        compiler_params=params(has_side_effects=True, collective_id=0, vmem_limit_bytes=17 << 20),
    )(
        *[
            pltpu.with_memory_space_constraint(value, pltpu.HBM)
            for value in (points, charges, projection, skeleton_index, near_ids.T, far_ids.T)
        ]
    )
    tables = [table, y_table, x_aug.reshape(targets, 64, cols), w_table]
    partial_sums = pl.pallas_call(
        pair_kernel,
        out_shape=pltpu.VMEM((targets + 1, rhs, cols), F32),
        in_specs=[VMEM] * 4,
        out_specs=VMEM,
        scratch_shapes=[
            pltpu.VMEM((DUOS, skel, 2 * cols), F32),
            pltpu.VMEM((DUOS, skel, 2 * cols), F32),
            pltpu.SMEM((chips * n_z, 128), jnp.int32),
            pltpu.SMEM((chips * n_z * (2 * NEAR_SLOTS + FAR_SLOTS) + 8 * DUOS,), jnp.int32),
            dma,
        ],
        name="pairs",
        compiler_params=params(vmem_limit_bytes=6 << 20),
    )(*[pltpu.with_memory_space_constraint(value, pltpu.VMEM) for value in tables])
    half, part = leaf_dev // 2, leaf_dev // 4
    return pl.pallas_call(
        functools.partial(reduce_kernel, leaf_dev),
        out_shape=pltpu.VMEM((leaf_dev, rhs, cols), F32),
        in_specs=[VMEM],
        out_specs=VMEM,
        scratch_shapes=[
            pltpu.VMEM((20, part, rhs, cols), jnp.int16),
            pltpu.VMEM((20, part, rhs, cols), jnp.int16),
            pltpu.VMEM((20, half, rhs, cols), jnp.int16),
            pltpu.VMEM((20, half, rhs, cols), jnp.int16),
            pltpu.VMEM((20, part, cols), F32),
            pltpu.VMEM((20, part, cols), F32),
            pltpu.VMEM((20, half, cols), F32),
            pltpu.VMEM((20, half, cols), F32),
            dma((40,)), dma((40,)), dma((40,)), dma((40,)),
        ],
        name="reduce",
        compiler_params=params(has_side_effects=True, collective_id=1, vmem_limit_bytes=17 << 20),
    )(pltpu.with_memory_space_constraint(partial_sums, pltpu.VMEM))


def solution(mesh):
    in_specs = (
        P("leaf", None, None),
        P("leaf", None, None),
        P("leaf", "nbr", None),
        P("leaf", None),
        P("leaf", "nbr"),
        P("leaf", "nbr"),
    )
    out_specs = P("leaf", None, "nbr")
    return jax.shard_map(per_device, mesh=mesh, in_specs=in_specs, out_specs=out_specs, check_vma=False)
```

```python
import functools
import math

import jax
import jax.numpy as jnp
from jax import lax
from jax.experimental import pallas as pl
from jax.experimental.pallas import tpu as pltpu
from jax.sharding import PartitionSpec as P

MESH = pl.DeviceIdType.MESH
HBM = pl.BlockSpec(memory_space=pltpu.HBM)
VMEM = pl.BlockSpec(memory_space=pltpu.VMEM)
RING = 4
NEAR_SLOTS = 6
FAR_SLOTS = 10
DUOS = 8
F32 = jnp.float32
BF16 = jnp.bfloat16


def torus_position():
    leaf = lax.axis_index("leaf")
    chip = leaf // 2
    return chip // RING, chip % RING, leaf % 2, lax.axis_index("nbr")


def wrap(value):
    return lax.rem(value + 2 * RING, RING)


def pick(first_is_x, u, v):
    return u * RING + v if first_is_x else v * RING + u


def chip_table(leaf_dev, near_dev, far_dev, n_z, chip, core, ids_all):
    rows = ids_all.shape[0]
    lane = lax.broadcasted_iota(jnp.int32, (rows, 128), 1)
    row = lax.broadcasted_iota(jnp.int32, (rows, 128), 0)
    upper = lax.broadcasted_iota(jnp.int32, (128, 128), 0) <= lax.broadcasted_iota(jnp.int32, (128, 128), 1)
    upper = jnp.where(upper, 1.0, 0.0).astype(BF16)
    result = jnp.zeros((rows, 128), jnp.int32)
    for at, (per_leaf, slots, start) in enumerate(((near_dev, NEAR_SLOTS, 0), (far_dev, FAR_SLOTS, NEAR_SLOTS))):
        first = 0 if at == 0 else near_dev
        pieces = [ids_all[:, first + step, :leaf_dev] for step in range(per_leaf)]
        if per_leaf * leaf_dev < 128:
            pieces.append(jnp.full((rows, 128 - per_leaf * leaf_dev), -1, jnp.int32))
        ids = jnp.concatenate(pieces, axis=1)
        named = lax.div(ids, 2 * leaf_dev)
        member = jnp.logical_and(named == chip, ids >= 0)
        source = lax.rem(lax.rem(ids, 2 * leaf_dev) + core * leaf_dev, 2 * leaf_dev)
        code = (lax.div(row, n_z) * leaf_dev + lax.rem(lane, leaf_dev)) * 256 + source + at * 4 * leaf_dev
        flags = jnp.where(member, 1.0, 0.0)
        upto = jnp.dot(flags.astype(BF16), upper, preferred_element_type=F32).astype(jnp.int32)
        for slot in range(slots):
            chosen = jnp.logical_and(member, upto == slot + 1)
            value = jnp.sum(jnp.where(chosen, code, 0), axis=1, keepdims=True)
            result = jnp.where(lane == start + slot, value, result)
        count = jnp.sum(jnp.where(member, 1, 0), axis=1, keepdims=True)
        result = jnp.where(lane == NEAR_SLOTS + FAR_SLOTS + at, count, result)
    return result


def norm_rows(coords, sign_first):
    values = coords.astype(F32)
    norm = -jnp.sum(values * values, axis=0, keepdims=True)
    high = norm.astype(BF16).astype(F32)
    rest = norm - high
    middle = rest.astype(BF16).astype(F32)
    low = rest - middle
    shape = (16, coords.shape[1])
    row = lax.broadcasted_iota(jnp.int32, shape, 0)
    start = 0 if sign_first else 3
    ones = 3 if sign_first else 0
    result = jnp.where(jnp.logical_and(row >= ones, row < ones + 3), 1.0, 0.0)
    for at, piece in enumerate((high, middle, low)):
        result = jnp.where(row == start + at, jnp.broadcast_to(piece, shape), result)
    return result.astype(BF16)


def gather_kernel(
    points, charges, projection, index, near_in, far_in,
    y_table, x_aug, w_table, table,
    near_t, far_t, ids, ids_all, p_buf, i_buf, c_buf, j_buf, q_buf, x_raw,
    send_x, recv_x, send_s, recv_s, send_i, recv_i, load_sems,
):
    x, y, core, z = torus_position()
    n_z = q_buf.shape[1]
    near_dev, far_dev = near_t.shape[0], far_t.shape[0]
    leaf_dev, dim, leaf = points.shape
    skel = index.shape[1]
    cols = x_raw.shape[3]
    half, part = leaf_dev // 2, leaf_dev // 4
    hold = leaf_dev // 2
    piece = skel // n_z
    me = (x * RING + y) * n_z + z
    n_ids = ids_all.shape[0]
    here = x * RING + y
    own_cols = pl.ds(pl.multiple_of(z * cols, cols), cols)

    def device(chip, core_at, z_at):
        return (chip * 2 + core_at, z_at)

    barrier = pltpu.get_barrier_semaphore()

    peers = []
    for dx in range(RING):
        for dy in range(RING):
            chip = wrap(x + dx) * RING + wrap(y + dy)
            for dz in range(n_z):
                if dx or dy or dz:
                    peers.append(device(chip, core, lax.rem(z + dz, n_z)))
    for peer in peers:
        pl.semaphore_signal(barrier, inc=1, device_id=peer, device_id_type=MESH)
    pl.semaphore_signal(barrier, inc=1, device_id=device(here, 1 - core, z), device_id_type=MESH)

    loads = []
    for at, (src, dst) in enumerate(
        (
            (charges, c_buf),
            (projection, j_buf),
            (points, p_buf.at[0]),
            (index, i_buf.at[0]),
            (points.at[:, :, own_cols], x_raw.at[here]),
            (charges.at[:, :, pl.ds(0, skel)], w_table.at[pl.ds(0, leaf_dev)]),
            (charges.at[:, :, pl.ds(skel, skel)], w_table.at[pl.ds(2 * leaf_dev, leaf_dev)]),
            (near_in, near_t),
            (far_in, far_t),
        )
    ):
        copy = pltpu.make_async_copy(src, dst, load_sems.at[at])
        copy.start()
        loads.append(copy)

    blank = jnp.full(ids.shape, -1, jnp.int32)
    ids[...] = blank
    loads[7].wait()
    loads[8].wait()
    ids[:near_dev, :leaf_dev] = near_t[...]
    ids[near_dev : near_dev + far_dev, :leaf_dev] = far_t[...]

    loads[0].wait()
    loads[1].wait()

    def charge(item, carry):
        parts = []
        for at in (item, item + hold):
            parts.append(
                lax.dot_general(c_buf[at], j_buf[at], (((1,), (1,)), ((), ())), preferred_element_type=F32)
            )
        q_buf[0, z, item] = jnp.concatenate(parts, axis=1).astype(BF16)
        return carry

    lax.fori_loop(0, hold, charge, 0, unroll=2)
    pl.semaphore_wait(barrier, n_ids)
    sends = []

    def message(kind, sems, src, dst, target):
        return pltpu.make_async_remote_copy(
            src_ref=src, dst_ref=dst, send_sem=sems[0].at[kind], recv_sem=sems[1].at[kind],
            device_id=target, device_id_type=MESH,
        )

    def start(copy):
        copy.start()
        sends.append(copy)

    side = (send_s, recv_s)
    line = (send_x, recv_x)

    own_x = []
    for half_at in range(2):
        first_x = half_at == 0
        u, v = (x, y) if first_x else (y, x)
        rows = pl.ds(half_at * half, half)
        src = points.at[rows, :, own_cols]
        dst = x_raw.at[here, rows]
        kinds = 20 * half_at
        own_x.append(
            [
                message(kinds + 0, line, src, dst, device(pick(first_x, wrap(u + 1), v), core, z)),
                message(kinds + 1, line, src, dst, device(pick(first_x, wrap(u - 1), v), core, z)),
                message(kinds + 4, line, src, dst, device(pick(first_x, u, wrap(v + 1)), core, z)),
                message(kinds + 5, line, src, dst, device(pick(first_x, u, wrap(v - 1)), core, z)),
            ]
        )
    for at in range(4):
        for half_at in range(2):
            start(own_x[half_at][at])

    sib_copies = []
    for at, (src, dst) in enumerate(
        (
            (points, p_buf.at[1]),
            (index, i_buf.at[1]),
            (charges.at[:, :, pl.ds(0, skel)], w_table.at[pl.ds(leaf_dev, leaf_dev)]),
            (charges.at[:, :, pl.ds(skel, skel)], w_table.at[pl.ds(3 * leaf_dev, leaf_dev)]),
        )
    ):
        copy = message(8 + at, side, src, dst, device(here, 1 - core, z))
        start(copy)
        sib_copies.append(copy)

    z_copies = []
    own_quarter = q_buf.at[0, z]
    for step in range(1, n_z):
        copy = message(step, side, own_quarter, own_quarter, device(here, core, lax.rem(z + step, n_z)))
        start(copy)
        z_copies.append(copy)
    copy = message(0, side, own_quarter, q_buf.at[1, z], device(here, 1 - core, z))
    start(copy)
    sib_quarters = [copy]

    for peer in peers:
        pltpu.make_async_remote_copy(
            src_ref=ids, dst_ref=ids_all.at[me], send_sem=send_i, recv_sem=recv_i,
            device_id=peer, device_id_type=MESH,
        ).start()

    def item(half_at, du, dv, quarter_at=None):
        first_x = half_at == 0
        u, v = (x, y) if first_x else (y, x)
        rows = pl.ds(half_at * half, half) if quarter_at is None else pl.ds(half_at * half + quarter_at * part, part)
        return x_raw.at[pick(first_x, wrap(u + du), wrap(v + dv)), rows]

    def target(half_at, du, dv):
        first_x = half_at == 0
        u, v = (x, y) if first_x else (y, x)
        return device(pick(first_x, wrap(u + du), wrap(v + dv)), core, z)

    def arrived(half_at, kind, ref):
        message(20 * half_at + kind, line, ref, ref, target(half_at, 1, 0)).wait_recv()

    def forward(half_at, kind, ref, du, dv):
        start(message(20 * half_at + kind, line, ref, ref, target(half_at, du, dv)))

    def across(half_at, slot, du):
        ref = item(half_at, du, 0)
        forward(half_at, 4 + 4 * slot, ref, 0, 1)
        forward(half_at, 5 + 4 * slot, ref, 0, -1)

    def relay(half_at, slot, du):
        arrived(half_at, 4 + 4 * slot, item(half_at, du, -1))
        forward(half_at, 6 + 4 * slot, item(half_at, du, -1, 0), 0, 1)
        arrived(half_at, 5 + 4 * slot, item(half_at, du, 1))
        forward(half_at, 7 + 4 * slot, item(half_at, du, 1, 1), 0, -1)

    pad = jnp.zeros((16, cols), BF16)

    def widen(half_at, du, dv):
        first_x = half_at == 0
        u, v = (x, y) if first_x else (y, x)
        chip = pick(first_x, wrap(u + du), wrap(v + dv))
        base = half_at * half

        def body(at, carry):
            coords = x_raw[chip, base + at]
            x_aug[chip, base + at] = jnp.concatenate([coords, norm_rows(coords, True), pad], axis=0)
            return carry

        lax.fori_loop(0, half, body, 0, unroll=4)

    wide_pad = jnp.zeros((16, leaf), BF16)
    point_number = lax.broadcasted_iota(jnp.int32, (leaf, skel), 0)
    sources = 2 * leaf_dev

    def source(at_side, first, count):
        def body(at, carry):
            coords = p_buf[at_side, at]
            block = jnp.concatenate([coords + coords, norm_rows(coords, False), wide_pad], axis=0)
            block = jnp.concatenate([block, block], axis=0)
            turned = block.T
            row = at_side * leaf_dev + at
            y_table[row] = turned[:skel]
            y_table[sources + row] = turned[skel:]
            chosen = point_number == i_buf[at_side, pl.ds(at, 1), :]
            chosen = jnp.where(chosen, 1.0, 0.0).astype(BF16)
            picked = jnp.dot(block, chosen, preferred_element_type=F32).astype(BF16)
            y_table[2 * sources + row] = picked.T
            return carry

        lax.fori_loop(first, first + count, body, 0, unroll=4)

    def assemble(at_side):
        def body(at, carry):
            chunks = [q_buf[at_side, step, at] for step in range(n_z)]
            for half_at in range(2):
                pieces = [chunk[:, half_at * piece : (half_at + 1) * piece] for chunk in chunks]
                w_table[2 * sources + at_side * leaf_dev + half_at * hold + at] = jnp.concatenate(pieces, axis=1)
            return carry

        lax.fori_loop(0, hold, body, 0, unroll=2)

    for copy in loads[2:5]:
        copy.wait()
    source(0, 0, leaf_dev // 2)
    for half_at in range(2):
        arrived(half_at, 0, item(half_at, -1, 0))
        forward(half_at, 2, item(half_at, -1, 0, 0), 1, 0)
        across(half_at, 1, -1)
    for half_at in range(2):
        arrived(half_at, 1, item(half_at, 1, 0))
        forward(half_at, 3, item(half_at, 1, 0, 1), -1, 0)
        across(half_at, 2, 1)
    source(0, leaf_dev // 2, leaf_dev // 2)
    for half_at in range(2):
        relay(half_at, 0, 0)
    for step in range(1, n_z):
        z_copies[step - 1].wait_recv()
        slot = lax.rem(z - step + n_z, n_z)
        copy = message(4 + step, side, q_buf.at[0, slot], q_buf.at[1, slot], device(here, 1 - core, z))
        start(copy)
        sib_quarters.append(copy)
    sib_copies[0].wait_recv()
    sib_copies[1].wait_recv()
    source(1, 0, leaf_dev // 2)
    for half_at in range(2):
        arrived(half_at, 2, item(half_at, 2, 0, 0))
        arrived(half_at, 3, item(half_at, 2, 0, 1))
        across(half_at, 3, 2)
    source(1, leaf_dev // 2, leaf_dev // 2)
    for half_at in range(2):
        relay(half_at, 1, -1)
    for half_at in range(2):
        for du in (0, -1, 1, 2):
            widen(half_at, du, 0)
    for half_at in range(2):
        relay(half_at, 2, 1)
    for copy in loads[5:7]:
        copy.wait()
    sib_copies[2].wait_recv()
    sib_copies[3].wait_recv()
    assemble(0)
    for copy in sib_quarters:
        copy.wait_recv()
    assemble(1)
    for half_at in range(2):
        relay(half_at, 3, 2)
    ids_all[me] = ids[...]
    others = ids_all.at[pl.ds(0, n_ids - 1)]
    every = pltpu.make_async_remote_copy(
        src_ref=others, dst_ref=others, send_sem=send_i, recv_sem=recv_i,
        device_id=target(0, 1, 0), device_id_type=MESH,
    )
    every.wait_send()
    every.wait_recv()
    table[...] = chip_table(leaf_dev, near_dev, far_dev, n_z, here, core, ids_all)
    for half_at in range(2):
        for dv in (-1, 1):
            for du in (0, -1, 1, 2):
                widen(half_at, du, dv)
    for slot, du in ((0, 0), (1, -1), (2, 1), (3, 2)):
        for half_at in range(2):
            arrived(half_at, 6 + 4 * slot, item(half_at, du, 2, 0))
            arrived(half_at, 7 + 4 * slot, item(half_at, du, 2, 1))
            widen(half_at, du, 2)
    for copy in sends:
        copy.wait_send()


def pair_kernel(table_in, y_table, x_aug, w_table, acc, s_a, s_b, table, items, load_sem):
    copy = pltpu.make_async_copy(table_in, table, load_sem)
    copy.start()
    skel = y_table.shape[1]
    targets, _, cols = x_aug.shape
    leaf_dev = w_table.shape[0] // 6
    n_z = table.shape[0] // (targets // leaf_dev)
    sources = 2 * leaf_dev

    blank = jnp.zeros((leaf_dev,) + acc.shape[1:], F32)
    acc[targets] = blank[0]
    copy.wait()

    def fill(chip, count):
        acc[pl.ds(pl.multiple_of(chip * leaf_dev, leaf_dev), leaf_dev)] = blank
        for step in range(n_z):
            row = chip * n_z + step
            for slot in range(NEAR_SLOTS):
                code = table[row, slot]
                items[count + 2 * slot] = code
                items[count + 2 * slot + 1] = code + sources
            count = count + 2 * table[row, NEAR_SLOTS + FAR_SLOTS]
            for slot in range(FAR_SLOTS):
                items[count + slot] = table[row, NEAR_SLOTS + slot]
            count = count + table[row, NEAR_SLOTS + FAR_SLOTS + 1]
        return count

    chips = table.shape[0] // n_z
    count = lax.fori_loop(0, chips, fill, 0)
    for at in range(6 * DUOS):
        items[count + at] = targets * 256


    empty = jnp.zeros((64, cols), BF16)
    low_lanes = lax.broadcasted_iota(jnp.int32, (skel, 128), 1) < 64

    def read(at):
        code = items[at]
        return lax.shift_right_logical(code, 8), jnp.bitwise_and(code, 255)

    def scores(group, buf, at):
        for duo in [at]:
            t_0, u_0 = read(group * 2 * DUOS + 2 * duo)
            t_1, u_1 = read(group * 2 * DUOS + 2 * duo + 1)
            x_0 = x_aug[jnp.minimum(t_0, targets - 1)]
            x_1 = x_aug[jnp.minimum(t_1, targets - 1)]
            right = jnp.concatenate(
                [jnp.concatenate([x_0, empty], axis=0), jnp.concatenate([empty, x_1], axis=0)], axis=1
            )
            left = jnp.where(low_lanes, y_table[u_0], y_table[u_1])
            buf[duo] = jnp.dot(left, right, preferred_element_type=F32)

    def sums(group, buf, at):
        for duo in [at]:
            t_0, u_0 = read(group * 2 * DUOS + 2 * duo)
            t_1, u_1 = read(group * 2 * DUOS + 2 * duo + 1)
            kernel = jnp.exp(buf[duo]).astype(BF16)
            weights = jnp.concatenate([w_table[u_0], w_table[u_1]], axis=0)
            terms = jnp.dot(weights, kernel, preferred_element_type=F32)
            rhs = terms.shape[0] // 2
            acc[t_0] = acc[t_0] + terms[:rhs, :cols]
            acc[t_1] = acc[t_1] + terms[rhs:, cols:]

    for duo in range(DUOS):
        scores(0, s_a, duo)

    def step(at, carry):
        for duo in range(DUOS):
            sums(2 * at, s_a, duo)
            scores(2 * at + 1, s_b, duo)
        for duo in range(DUOS):
            sums(2 * at + 1, s_b, duo)
            scores(2 * at + 2, s_a, duo)
        return carry

    lax.fori_loop(0, lax.div(count + 4 * DUOS - 1, 4 * DUOS), step, 0)


def reduce_kernel(
    leaf_dev, held, out, send_8, recv_8, send_16, recv_16, scale_s8, scale_r8, scale_s16, scale_r16,
    sem_s8, sem_r8, sem_s16, sem_r16,
):
    x, y, core, z = torus_position()
    half, part = leaf_dev // 2, leaf_dev // 4
    order = ((2, 0), (1, 1), (-1, 2), (0, 3))

    def chip_at(half_at, du, dv):
        first_x = half_at == 0
        u, v = (x, y) if first_x else (y, x)
        return pick(first_x, wrap(u + du), wrap(v + dv))

    barrier = pltpu.get_barrier_semaphore()
    for du, dv in ((1, 0), (-1, 0), (0, 1), (0, -1)):
        pl.semaphore_signal(
            barrier, inc=1, device_id=(chip_at(0, du, dv) * 2 + core, z), device_id_type=MESH
        )

    pl.semaphore_wait(barrier, 4)
    sends = []

    def wires(size, kind, chip):
        big = size == half
        pairs = (
            ((send_16, recv_16, sem_s16, sem_r16, 0), (scale_s16, scale_r16, sem_s16, sem_r16, 1))
            if big
            else ((send_8, recv_8, sem_s8, sem_r8, 0), (scale_s8, scale_r8, sem_s8, sem_r8, 1))
        )
        return [
            pltpu.make_async_remote_copy(
                src_ref=src.at[kind], dst_ref=dst.at[kind], send_sem=s.at[2 * kind + at], recv_sem=r.at[2 * kind + at],
                device_id=(chip * 2 + core, z), device_id_type=MESH,
            )
            for src, dst, s, r, at in pairs
        ]

    def unpack(size, kind, row):
        data, scale = (recv_16, scale_r16) if size == half else (recv_8, scale_r8)
        return data[kind, row].astype(jnp.int32).astype(F32) * scale[kind, pl.ds(row, 1), :]

    def code(size, kind, first, count, value_at):
        data, scale = (send_16, scale_s16) if size == half else (send_8, scale_s8)

        def body(row, carry):
            value = value_at(row)
            top = jnp.maximum(jnp.max(jnp.abs(value), axis=0, keepdims=True), 1e-30)
            scale[kind, pl.ds(row, 1), :] = top * (1.0 / 32767.0)
            data[kind, row] = jnp.round(value * (32767.0 / top)).astype(jnp.int32).astype(jnp.int16)
            return carry

        lax.fori_loop(first, first + count, body, 0, unroll=2)

    def send(size, kind, chip):
        for copy in wires(size, kind, chip):
            copy.start()
            sends.append(copy)

    def wait(size, kind):
        for copy in wires(size, kind, chip_at(0, 1, 0)):
            copy.wait_recv()

    def local(half_at, du, dv):
        start = chip_at(half_at, du, dv) * leaf_dev + half_at * half
        return lambda row: held[start + row]

    for dv, at in order:
        for half_at in range(2):
            kind = half_at * 10 + 2 * at
            mine = local(half_at, 2, dv)
            for side, du in ((0, 1), (1, -1)):
                code(part, kind + side, 0, part, lambda row: mine(side * part + row))
                send(part, kind + side, chip_at(half_at, du, 0))

    def add_part(kind, side, mine):
        wait(part, kind)
        low = side * part
        code(half, kind, low, part, lambda row: mine(row) + unpack(part, kind, row - low))

    def pass_on(dv, at):
        for half_at in range(2):
            for du, side in ((1, 0), (-1, 1)):
                kind = half_at * 10 + 2 * at + side
                mine = local(half_at, du, dv)
                code(half, kind, part - side * part, part, mine)
                add_part(kind, side, mine)
                send(half, kind, chip_at(half_at, du, 0))

    def column(half_at, dv, at):
        kind = half_at * 10 + 2 * at
        mine = local(half_at, 0, dv)
        wait(half, kind)
        wait(half, kind + 1)
        return lambda row: mine(row) + unpack(half, kind, row) + unpack(half, kind + 1, row)

    def second_axis(dv, at):
        for half_at in range(2):
            total = column(half_at, dv, at)
            if dv == 2:
                for sign, side in ((1, 0), (-1, 1)):
                    late = half_at * 10 + 8 + side
                    code(part, late, 0, part, lambda row: total(side * part + row))
                    send(part, late, chip_at(half_at, 0, sign))
            else:
                side = 0 if dv == 1 else 1
                late = half_at * 10 + 8 + side
                code(half, late, part - side * part, part, total)
                add_part(late, side, total)
                send(half, late, chip_at(half_at, 0, dv))

    for step, (dv, at) in enumerate(order):
        pass_on(dv, at)
        if step > 0:
            second_axis(*order[step - 1])
    for half_at in range(2):
        base = half_at * half
        total = column(half_at, *order[-1])
        kind = half_at * 10 + 8
        wait(half, kind)
        wait(half, kind + 1)

        def finish(row, carry):
            out[base + row] = total(row) + unpack(half, kind, row) + unpack(half, kind + 1, row)
            return carry

        lax.fori_loop(0, half, finish, 0, unroll=2)
    for copy in sends:
        copy.wait_send()


def per_device(points, charges, projection, skeleton_index, near_ids, far_ids):
    leaf_dev, dim, leaf = points.shape
    rhs = charges.shape[1]
    skel = skeleton_index.shape[1]
    n_z = lax.axis_size("nbr")
    chips = lax.axis_size("leaf") // 2
    cols = leaf // n_z
    near_dev, far_dev = near_ids.shape[1], far_ids.shape[1]
    sources, targets = 2 * leaf_dev, chips * leaf_dev
    params = pltpu.CompilerParams
    dma = pltpu.SemaphoreType.DMA
    shape = jax.ShapeDtypeStruct

    quarter = (leaf_dev // 2, rhs, 2 * skel // n_z)
    y_table, x_aug, w_table, table = pl.pallas_call(
        gather_kernel,
        out_shape=[
            pltpu.VMEM((3 * sources, skel, 128), BF16),
            pltpu.VMEM((chips, leaf_dev, 64, cols), BF16),
            pltpu.VMEM((3 * sources, rhs, skel), BF16),
            pltpu.VMEM((chips * n_z, 128), jnp.int32),
        ],
        in_specs=[HBM] * 6,
        out_specs=[VMEM] * 4,
        scratch_shapes=[
            pltpu.VMEM((near_dev, leaf_dev), jnp.int32),
            pltpu.VMEM((far_dev, leaf_dev), jnp.int32),
            pltpu.VMEM((8, 128), jnp.int32),
            pltpu.VMEM((chips * n_z, 8, 128), jnp.int32),
            pltpu.VMEM((2,) + points.shape, BF16),
            pltpu.VMEM((2,) + skeleton_index.shape, jnp.int32),
            pltpu.VMEM(charges.shape, BF16),
            pltpu.VMEM(projection.shape, BF16),
            pltpu.VMEM((2, n_z) + quarter, BF16),
            pltpu.VMEM((chips, leaf_dev, dim, cols), BF16),
            dma((40,)), dma((40,)), dma((12,)), dma((12,)), dma, dma, dma((9,)),
        ],
        name="gather",
        compiler_params=params(has_side_effects=True, collective_id=0, vmem_limit_bytes=17 << 20),
    )(
        *[
            pltpu.with_memory_space_constraint(value, pltpu.HBM)
            for value in (points, charges, projection, skeleton_index, near_ids.T, far_ids.T)
        ]
    )
    tables = [table, y_table, x_aug.reshape(targets, 64, cols), w_table]
    partial_sums = pl.pallas_call(
        pair_kernel,
        out_shape=pltpu.VMEM((targets + 1, rhs, cols), F32),
        in_specs=[VMEM] * 4,
        out_specs=VMEM,
        scratch_shapes=[
            pltpu.VMEM((DUOS, skel, 2 * cols), F32),
            pltpu.VMEM((DUOS, skel, 2 * cols), F32),
            pltpu.SMEM((chips * n_z, 128), jnp.int32),
            pltpu.SMEM((chips * n_z * (2 * NEAR_SLOTS + FAR_SLOTS) + 8 * DUOS,), jnp.int32),
            dma,
        ],
        name="pairs",
        compiler_params=params(vmem_limit_bytes=6 << 20),
    )(*[pltpu.with_memory_space_constraint(value, pltpu.VMEM) for value in tables])
    half, part = leaf_dev // 2, leaf_dev // 4
    return pl.pallas_call(
        functools.partial(reduce_kernel, leaf_dev),
        out_shape=pltpu.VMEM((leaf_dev, rhs, cols), F32),
        in_specs=[VMEM],
        out_specs=VMEM,
        scratch_shapes=[
            pltpu.VMEM((20, part, rhs, cols), jnp.int16),
            pltpu.VMEM((20, part, rhs, cols), jnp.int16),
            pltpu.VMEM((20, half, rhs, cols), jnp.int16),
            pltpu.VMEM((20, half, rhs, cols), jnp.int16),
            pltpu.VMEM((20, part, cols), F32),
            pltpu.VMEM((20, part, cols), F32),
            pltpu.VMEM((20, half, cols), F32),
            pltpu.VMEM((20, half, cols), F32),
            dma((40,)), dma((40,)), dma((40,)), dma((40,)),
        ],
        name="reduce",
        compiler_params=params(has_side_effects=True, collective_id=1, vmem_limit_bytes=17 << 20),
    )(pltpu.with_memory_space_constraint(partial_sums, pltpu.VMEM))


def solution(mesh):
    in_specs = (
        P("leaf", None, None),
        P("leaf", None, None),
        P("leaf", "nbr", None),
        P("leaf", None),
        P("leaf", "nbr"),
        P("leaf", "nbr"),
    )
    out_specs = P("leaf", None, "nbr")
    return jax.shard_map(per_device, mesh=mesh, in_specs=in_specs, out_specs=out_specs, check_vma=False)
```
